128 devices in a mesh: dp: 8 (over y, core), expert: 16 (over z, x).
Axes of the slice: x: 4, y: 4, z: 4, core: 2. Of those that a mesh axis runs over, the one named last changes fastest.
Arguments:
- tokens: bfloat16 [32768, 2048], P(('dp', 'expert')), may hold values from -6 to 6
- routes: int32 [32768, 2], P(('dp', 'expert')), may hold values from 0 to 31, all different within a row; in each aligned block of 256 rows (0 to 255, 256 to 511, ...) at most 32 rows name the same one
- gate_weights: float32 [32768, 2], P(('dp', 'expert')), may hold values from 0.2 to 1
- w_up: bfloat16 [32, 2048, 768], P('expert'), may hold values from -0.125 to 0.125
- w_down: bfloat16 [32, 768, 2048], P('expert'), may hold values from -0.21875 to 0.21875
- cotangent: bfloat16 [32768, 2048], P(('dp', 'expert')), may hold values from -6 to 6
Outputs:
- mixed: bfloat16 [32768, 2048], P(('dp', 'expert'))
- input_grad: bfloat16 [32768, 2048], P(('dp', 'expert'))
- up_grad: float32 [32, 2048, 768], P('expert', 'dp')
- down_grad: float32 [32, 768, 2048], P('expert', None, 'dp')
The draws below stay inside these ranges and needn't reach their ends.
Inputs may be any that keep to these rules, and one draw needn't show every extreme that they name: Each row names 2 different experts. In the rows of one device no expert is named by more than 32 routes, and in every draw some expert is named by exactly 32 routes of some device.
All inputs are finite; a program needn't handle non-finite values.
Results may differ from the reference program's by a relative error of at most 0.015.
Values may be sent and summed in bfloat16 or wider, within the bound.
A program may use at most 192 MiB of HBM per device.

```python
import math
import jax
import jax.numpy as jnp
import numpy as np
from jax import lax

D = 2048
FF = 768
TOP = 2
TOK_DEV = 256
EXPERTS = 32
CAP = 32
TOKENS = 32768
N_DP = 8
N_EXPERT = 16


def block_scale(own_key, shape, cuts, least, largest):
    loudness = 1.0
    for dim, blocks in cuts:
        draws = jax.random.uniform(jax.random.fold_in(jax.random.fold_in(own_key, 6), dim), (blocks,), jnp.float32, least / len(cuts), largest / len(cuts))
        loudness = loudness * jnp.repeat(jnp.exp(draws), shape[dim] // blocks).reshape((-1,) + (1,) * (len(shape) - 1 - dim))
    return loudness


def routed_block(key, own, number, rows, amount, top, limit, skew):
    ranking = jax.random.permutation(key, amount)
    crowded, usual = load_shares(amount, rows * top, limit, skew, True), load_shares(amount, rows * top, limit, skew, False)
    places = jnp.arange(amount)

    def named(sizes, turn):
        used = int((sizes > 0).sum())
        fixed = max(1, used // 4)
        shifted = fixed + (places - fixed + turn * (used - fixed)) % max(1, amount - fixed)
        return jnp.zeros((amount,), jnp.int32).at[ranking[jnp.where(places < fixed, places, shifted)]].set(jnp.asarray(sizes, jnp.int32))

    sizes = jnp.where(number % 4 == 0, named(crowded, number // 4), named(usual, number - number // 4 - 1))
    mixed = jax.random.permutation(jax.random.fold_in(own, 3), amount)
    source_of, receiver = mixed[0:amount // 2 * 2:2], mixed[1:amount // 2 * 2:2]
    room = jnp.minimum(sizes[source_of] - 1, limit - sizes[receiver]) // 2
    room = jnp.where((source_of == ranking[0]) | (receiver == ranking[0]) | (sizes[receiver] == 0), 0, jnp.maximum(room, 0))
    shifted = jax.random.randint(jax.random.fold_in(own, 4), (amount // 2,), 0, 1 << 20) % (room + 1)
    sizes = sizes.at[source_of].add(-shifted).at[receiver].add(shifted)
    labels = jnp.searchsorted(jnp.cumsum(sizes), jnp.arange(rows * top), side="right").astype(jnp.int32)
    grid = labels.reshape(top, rows).T
    grid = grid[jax.random.permutation(jax.random.fold_in(own, 1), rows)]
    turn = jax.random.randint(jax.random.fold_in(own, 2), (rows, 1), 0, top)
    return jnp.take_along_axis(grid, (jnp.arange(top)[None, :] + turn) % top, axis=1)


def load_shares(count, total, most, skew, full):
    loads = [(1 << 20) // math.isqrt(grade ** skew) + 1 for grade in range(1, count + 1)]
    largest = most if full else min(most, max(-(-total // count), total * loads[0] // sum(loads)))
    least = 1 if total - largest >= count - 1 else 0
    counts, spare = [largest] + [least] * (count - 1), total - largest - least * (count - 1)
    while spare > 0:
        candidates = [i for i in range(1, count) if counts[i] < largest] or [i for i in range(1, count) if counts[i] < most]
        pool, budget = sum([loads[i] for i in candidates]), spare
        for i in candidates:
            more = min(most - counts[i], max(1, budget * loads[i] // pool), spare)
            counts[i] = counts[i] + more
            spare = spare - more
    return np.array(counts)


def noise(rng, shape, spread, bound, cuts=(), kind=jnp.bfloat16):
    drawn = jax.random.normal(rng, shape, jnp.float32) * spread
    if len(cuts) > 0:
        drawn = block_scale(rng, shape, cuts, -0.22, 0.18) * drawn
    return jnp.clip(drawn, min=-bound, max=bound).astype(kind)


def setup_inputs(seed: int = 0) -> dict:
    splits = jax.random.split(jax.random.key(seed), 7)
    tokens = noise(splits[0], (TOKENS, D), 1.0, 6.0, ((0, 128),))
    routes_keys = jax.random.split(jax.random.fold_in(splits[1], 1), TOKENS // TOK_DEV)
    routes_turns = jax.random.permutation(jax.random.fold_in(splits[1], 3), TOKENS // TOK_DEV)
    routes = jax.vmap(lambda own, number: routed_block(jax.random.fold_in(splits[1], 2), own, number, TOK_DEV, EXPERTS, TOP, CAP, 2))(routes_keys, routes_turns).reshape((TOKENS, TOP))
    gate_weights = jnp.clip(0.2 + 0.8 * jax.random.uniform(splits[2], (TOKENS, TOP), jnp.float32) ** block_scale(splits[2], (TOKENS, TOP), ((0, 128),), -0.2, 0.2), 0.2, 1.0)
    w_up = noise(splits[3], (EXPERTS, D, FF), D ** -0.5, 0.125, ((0, 16),))
    w_down = noise(splits[4], (EXPERTS, FF, D), FF ** -0.5, 0.21875, ((0, 16),))
    cotangent = noise(splits[5], (TOKENS, D), 1.0, 6.0, ((0, 128),))
    return {"tokens": tokens, "routes": routes, "gate_weights": gate_weights, "w_up": w_up, "w_down": w_down, "cotangent": cotangent}


def route_slots(routes_dev, experts, capacity):
    flat_routes = routes_dev.reshape(-1)
    onehot = (flat_routes[:, None] == jnp.arange(experts, dtype=jnp.int32)[None, :]).astype(jnp.int32)
    before = jnp.cumsum(onehot, axis=0) - onehot
    position = jnp.sum(before * onehot, axis=1)
    return (flat_routes * capacity + position).astype(jnp.int32).reshape(routes_dev.shape)


def fill_slots(slot_index, pieces, slot_total):
    buffer = jnp.zeros((slot_total, pieces[0].shape[1]), jnp.bfloat16)
    for route_pick in range(len(pieces)):
        buffer = buffer.at[slot_index[:, route_pick]].set(pieces[route_pick])
    return buffer


def expert_pass(routed_rows, routed_cot, up_weight, down_weight):
    pre_act = jnp.dot(routed_rows, up_weight, preferred_element_type=jnp.float32)
    activated = jax.nn.silu(pre_act).astype(jnp.bfloat16)
    expert_out = jnp.dot(activated, down_weight, preferred_element_type=jnp.float32).astype(jnp.bfloat16)
    d_act = jnp.dot(routed_cot, down_weight.T, preferred_element_type=jnp.float32)
    sigmoid_pre = jax.nn.sigmoid(pre_act)
    d_pre = (d_act * sigmoid_pre * (1.0 + pre_act * (1.0 - sigmoid_pre))).astype(jnp.bfloat16)
    d_rows = jnp.dot(d_pre, up_weight.T, preferred_element_type=jnp.float32).astype(jnp.bfloat16)
    grad_up = jnp.dot(routed_rows.T, d_pre, preferred_element_type=jnp.float32).astype(jnp.bfloat16)
    grad_down = jnp.dot(activated.T, routed_cot, preferred_element_type=jnp.float32).astype(jnp.bfloat16)
    return expert_out, d_rows, grad_up, grad_down


def reference(tokens, routes, gate_weights, w_up, w_down, cotangent):
    slot_total = EXPERTS * CAP

    def device_pieces(slot_index, token_rows, gates, cot_rows):
        sent = fill_slots(slot_index, [token_rows] * TOP, slot_total)
        scaled = [(gates[:, pick:pick + 1] * cot_rows.astype(jnp.float32)).astype(jnp.bfloat16) for pick in range(TOP)]
        return sent, fill_slots(slot_index, scaled, slot_total)

    def by_expert(buffer):
        return buffer.reshape(N_EXPERT, EXPERTS, CAP, D).transpose(1, 0, 2, 3).reshape(EXPERTS, N_EXPERT * CAP, D)

    def by_source(buffer):
        return buffer.reshape(EXPERTS, N_EXPERT, CAP, D).transpose(1, 0, 2, 3).reshape(N_EXPERT, slot_total, D)

    def combine(slot_index, gates, returned, d_returned):
        mixed = jnp.zeros((TOK_DEV, D), jnp.float32)
        summed = jnp.zeros((TOK_DEV, D), jnp.float32)
        for pick in range(TOP):
            mixed = mixed + gates[:, pick:pick + 1] * returned[slot_index[:, pick]].astype(jnp.float32)
            summed = summed + d_returned[slot_index[:, pick]].astype(jnp.float32)
        return mixed.astype(jnp.bfloat16), summed.astype(jnp.bfloat16)

    def group_pass(grad_sums, group_data):
        tok_group, route_group, gate_group, cot_group = group_data
        slot_group = jax.vmap(lambda block: route_slots(block, EXPERTS, CAP))(route_group)
        sent, cot_sent = jax.vmap(device_pieces)(slot_group, tok_group, gate_group, cot_group)
        expert_out, d_rows, grad_up, grad_down = lax.map(
            lambda operands: expert_pass(*operands), (by_expert(sent), by_expert(cot_sent), w_up, w_down))
        mixed, input_grad = jax.vmap(combine)(slot_group, gate_group, by_source(expert_out), by_source(d_rows))
        grad_up = lax.optimization_barrier(grad_up)
        grad_down = lax.optimization_barrier(grad_down)
        new_sums = (grad_sums[0] + grad_up.astype(jnp.float32), grad_sums[1] + grad_down.astype(jnp.float32))
        return new_sums, (mixed, input_grad)

    start_sums = (jnp.zeros((EXPERTS, D, FF), jnp.float32), jnp.zeros((EXPERTS, FF, D), jnp.float32))
    group_data = (tokens.reshape(N_DP, N_EXPERT, TOK_DEV, D), routes.reshape(N_DP, N_EXPERT, TOK_DEV, TOP),
                  gate_weights.reshape(N_DP, N_EXPERT, TOK_DEV, TOP), cotangent.reshape(N_DP, N_EXPERT, TOK_DEV, D))
    grad_sums, stacked = lax.scan(group_pass, start_sums, group_data)
    mixed = stacked[0].reshape(TOKENS, D)
    input_grad = stacked[1].reshape(TOKENS, D)
    return (mixed, input_grad, grad_sums[0], grad_sums[1])
```

```python
import jax
import jax.numpy as jnp
from jax import lax
from jax.experimental import pallas as pl
from jax.experimental.pallas import tpu as pltpu
from jax.sharding import PartitionSpec as P

MESH = pl.DeviceIdType.MESH
SIDE = 4
CORES = 2
F32 = jnp.float32
BF16 = jnp.bfloat16


def dot(a, b, dims):
    return lax.dot_general(a, b, (dims, ((), ())), preferred_element_type=F32)


NN = ((1,), (0,))
NT = ((1,), (1,))
TN = ((0,), (0,))


def sigmoid(v):
    return 1.0 / (1.0 + jnp.exp(-v))


def step_of(j):
    return j ^ (j // 2)


def layer_kernel(
    tok_hbm, cot_hbm, routes, gates, wup_hbm, wdn_hbm,
    mixed_hbm, igrad_hbm, upg_hbm, dng_hbm,
    tokbuf, cotbuf, meta_z, meta_x, sbuf_t, sbuf_c, recv_t, recv_c, wu, wd,
    pre, act, dpre, ret_o, ret_d, rs, pmr, pdr, gst,
    load_sem, meta_sems, ag_send, ag_recv, meta_send, meta_recv,
    fwd_send, fwd_recv, bwd_send, bwd_recv, rs_send, rs_recv, part_send, part_recv, out_sem,
):
    dp, ex = lax.axis_index("dp"), lax.axis_index("expert")
    y, c = dp // CORES, dp % CORES
    z, x = ex // SIDE, ex % SIDE
    rows, width = tok_hbm.shape
    hidden = wup_hbm.shape[2]
    cap = rows // (SIDE * CORES)
    pair = CORES * cap
    tile = width // SIDE
    shard = width // (SIDE * CORES)
    line = SIDE * CORES
    mine = (x * CORES + c) * cap
    mine_z = (z * CORES + c) * cap

    def device(yy, cc, zz, xx):
        return (yy * CORES + cc, zz * SIDE + xx)

    def x_line(q):
        return (x + q // CORES) % SIDE, (c + q % CORES) % CORES

    def z_line(q):
        return (z + q // CORES) % SIDE, (c + q % CORES) % CORES

    def y_line(q):
        return (y + q // CORES) % SIDE, (c + q % CORES) % CORES

    def remote(src, dst, ssem, rsem, where):
        return pltpu.make_async_remote_copy(
            src_ref=src, dst_ref=dst, send_sem=ssem, recv_sem=rsem,
            device_id=where, device_id_type=MESH,
        )

    def await_bytes(ref, sem):
        pltpu.make_async_copy(ref, ref, sem).wait()

    tok_in = pltpu.make_async_copy(tok_hbm, tokbuf.at[z], load_sem.at[0])
    cot_in = pltpu.make_async_copy(cot_hbm, cotbuf.at[x], load_sem.at[1])
    wup_in = pltpu.make_async_copy(wup_hbm.at[c], wu, load_sem.at[2])
    wdn_in = pltpu.make_async_copy(wdn_hbm.at[c], wd, load_sem.at[3])
    tok_in.start()
    cot_in.start()

    barrier = pltpu.get_barrier_semaphore()

    def greet(where):
        pl.semaphore_signal(barrier, inc=1, device_id=where, device_id_type=MESH)

    @pl.loop(1, line)
    def _(q):
        xx, cc = x_line(q)
        greet(device(y, cc, z, xx))

    @pl.loop(CORES, line)
    def _(q):
        zz, cc = z_line(q)
        greet(device(y, cc, zz, x))
        yy, cc = y_line(q)
        greet(device(yy, cc, z, x))

    r0, r1 = routes[0:1, :], routes[1:2, :]
    experts = line * SIDE
    names = lax.broadcasted_iota(jnp.int32, (experts, rows), 0)
    hit0, hit1 = names == r0, names == r1
    onehot = jnp.where(hit0 | hit1, 1.0, 0.0).astype(BF16)
    earlier = (
        lax.broadcasted_iota(jnp.int32, (rows, rows), 0)
        < lax.broadcasted_iota(jnp.int32, (rows, rows), 1)
    )
    before = dot(onehot, jnp.where(earlier, 1.0, 0.0).astype(BF16), NN)
    slot0 = r0.astype(F32) * cap + jnp.sum(jnp.where(hit0, before, 0.0), axis=0, keepdims=True)
    slot1 = r1.astype(F32) * cap + jnp.sum(jnp.where(hit1, before, 0.0), axis=0, keepdims=True)
    meta = jnp.concatenate(
        [slot0, slot1, gates[0:1, :], gates[1:2, :], jnp.zeros((4, rows), F32)], axis=0
    )
    meta_z[z] = meta
    meta_x[x] = meta

    pl.semaphore_wait(barrier, line - 1 + 2 * (line - CORES))

    @pl.loop(1, SIDE)
    def _(j):
        d = step_of(j)
        to_z, to_x = device(y, c, (z + d) % SIDE, x), device(y, c, z, (x + d) % SIDE)
        remote(meta_z.at[z], meta_z.at[z], meta_send.at[0, d], meta_recv.at[0, z], to_z).start()
        remote(meta_x.at[x], meta_x.at[x], meta_send.at[1, d], meta_recv.at[1, x], to_x).start()

    tok_in.wait()
    cot_in.wait()

    @pl.loop(1, SIDE)
    def _(j):
        d = step_of(j)
        to_z, to_x = device(y, c, (z + d) % SIDE, x), device(y, c, z, (x + d) % SIDE)
        remote(tokbuf.at[z], tokbuf.at[z], ag_send.at[0, d], ag_recv.at[0, z], to_z).start()
        remote(cotbuf.at[x], cotbuf.at[x], ag_send.at[1, d], ag_recv.at[1, x], to_x).start()

    wup_in.start()
    wdn_in.start()

    place = lax.broadcasted_iota(jnp.int32, (rows, rows), 0)
    tok_slots = (place + z * rows).astype(F32)
    cot_slots = ((place // pair) * rows + x * pair + place % pair).astype(F32)

    @pl.loop(0, SIDE)
    def _(j):
        d = step_of(j)
        zs, xs = (z + d) % SIDE, (x + d) % SIDE

        @pl.when(j > 0)
        def _():
            await_bytes(meta_z.at[zs], meta_recv.at[0, zs])
            await_bytes(tokbuf.at[zs], ag_recv.at[0, zs])

        m = meta_z[zs]
        pick = jnp.where((tok_slots == m[0:1, :]) | (tok_slots == m[1:2, :]), 1.0, 0.0).astype(BF16)

        @pl.loop(0, SIDE)
        def _(n):
            cols = pl.ds(pl.multiple_of(n * tile, tile), tile)
            sbuf_t[zs, :, cols] = dot(pick, tokbuf[zs, :, cols], NN).astype(BF16)

        @pl.loop(1, line)
        def _(q):
            xx, cc = x_line(q)
            remote(
                sbuf_t.at[zs, pl.ds((xx * CORES + cc) * cap, cap)],
                recv_t.at[zs, pl.ds(mine, cap)],
                fwd_send.at[0, zs], fwd_recv.at[0, zs], device(y, cc, z, xx),
            ).start()

        pltpu.make_async_copy(
            sbuf_t.at[zs, pl.ds(mine, cap)], recv_t.at[zs, pl.ds(mine, cap)], fwd_recv.at[0, zs]
        ).start()

        @pl.when(j > 0)
        def _():
            await_bytes(meta_x.at[xs], meta_recv.at[1, xs])
            await_bytes(cotbuf.at[xs], ag_recv.at[1, xs])

        m = meta_x[xs]
        hit0, hit1 = cot_slots == m[0:1, :], cot_slots == m[1:2, :]
        pick = jnp.where(hit0 | hit1, 1.0, 0.0).astype(BF16)
        scale = jnp.sum(
            jnp.where(hit0, m[2:3, :], 0.0) + jnp.where(hit1, m[3:4, :], 0.0), axis=1, keepdims=True
        )

        @pl.loop(0, SIDE)
        def _(n):
            cols = pl.ds(pl.multiple_of(n * tile, tile), tile)
            sbuf_c[xs, :, cols] = (dot(pick, cotbuf[xs, :, cols], NN) * scale).astype(BF16)

        @pl.loop(1, line)
        def _(q):
            zz, cc = z_line(q)
            remote(
                sbuf_c.at[xs, pl.ds((zz * CORES + cc) * cap, cap)],
                recv_c.at[z, pl.ds((xs * CORES + c) * cap, cap)],
                fwd_send.at[1, xs], fwd_recv.at[1, xs], device(y, cc, zz, x),
            ).start()

        pltpu.make_async_copy(
            sbuf_c.at[xs, pl.ds(mine_z, cap)],
            recv_c.at[z, pl.ds((xs * CORES + c) * cap, cap)],
            fwd_recv.at[1, xs],
        ).start()

    wup_in.wait()
    wdn_in.wait()

    @pl.loop(0, SIDE)
    def _(j):
        zs = (z + step_of(j)) % SIDE
        await_bytes(recv_t.at[zs], fwd_recv.at[0, zs])
        v = dot(recv_t[zs], wu[...], NN)
        pre[zs] = v
        a = (v * sigmoid(v)).astype(BF16)
        act[zs] = a
        await_bytes(sbuf_t.at[zs, pl.ds(0, rows - cap)], fwd_send.at[0, zs])

        @pl.loop(0, SIDE)
        def _(n):
            cols = pl.ds(pl.multiple_of(n * tile, tile), tile)
            sbuf_t[zs, :, cols] = dot(act[zs], wd[:, cols], NN).astype(BF16)

        @pl.loop(1, line)
        def _(q):
            xx, cc = x_line(q)
            remote(
                sbuf_t.at[zs, pl.ds((xx * CORES + cc) * cap, cap)],
                ret_o.at[zs, pl.ds(mine, cap)],
                bwd_send.at[0, zs], bwd_recv.at[0, zs], device(y, cc, z, xx),
            ).start()

        pltpu.make_async_copy(
            sbuf_t.at[zs, pl.ds(mine, cap)], ret_o.at[zs, pl.ds(mine, cap)], bwd_recv.at[0, zs]
        ).start()

    @pl.loop(0, SIDE)
    def _(j):
        xs = (x + step_of(j)) % SIDE
        part = pl.ds(pl.multiple_of(xs * pair, pair), pair)
        await_bytes(recv_c.at[:, part], fwd_recv.at[1, xs])
        da = dot(recv_c[:, part, :].reshape(rows, width), wd[...], NT)
        v = pre[:, part, :].reshape(rows, hidden)
        s = sigmoid(v)
        dp_rows = (da * s * (1.0 + v * (1.0 - s))).astype(BF16)
        dpre[:, part, :] = dp_rows.reshape(SIDE, pair, hidden)
        await_bytes(sbuf_c.at[xs, pl.ds(0, rows - cap)], fwd_send.at[1, xs])

        @pl.loop(0, SIDE)
        def _(n):
            cols = pl.ds(pl.multiple_of(n * tile, tile), tile)
            left = dpre[:, part, :].reshape(rows, hidden)
            sbuf_c[xs, :, cols] = dot(left, wu[cols, :], NT).astype(BF16)

        @pl.loop(1, line)
        def _(q):
            zz, cc = z_line(q)
            remote(
                sbuf_c.at[xs, pl.ds((zz * CORES + cc) * cap, cap)],
                ret_d.at[xs, pl.ds(mine_z, cap)],
                bwd_send.at[1, xs], bwd_recv.at[1, xs], device(y, cc, zz, x),
            ).start()

        pltpu.make_async_copy(
            sbuf_c.at[xs, pl.ds(mine_z, cap)], ret_d.at[xs, pl.ds(mine_z, cap)], bwd_recv.at[1, xs]
        ).start()

    @pl.loop(1, SIDE)
    def _(d):
        for k, buf, own, metas in ((0, tokbuf, z, meta_z), (1, cotbuf, x, meta_x)):
            await_bytes(buf.at[own], ag_send.at[k, d])
            await_bytes(metas.at[own], meta_send.at[k, d])

    thirds = hidden // rows
    for g, left, right, gbuf in ((0, act, recv_c, cotbuf), (1, dpre, recv_t, tokbuf)):

        @pl.loop(0, SIDE)
        def _(n, g=g, left=left, right=right, gbuf=gbuf):
            yy = (y + step_of(SIDE - 1 - n)) % SIDE
            cols = pl.ds(pl.multiple_of(yy * tile, tile), tile)
            r = dot(
                left[...].reshape(SIDE * rows, hidden),
                right[:, :, cols].reshape(SIDE * rows, tile),
                TN,
            )
            gbuf[0:thirds, :, cols] = r.astype(BF16).reshape(thirds, rows, tile)

        @pl.loop(1, line)
        def _(q, g=g, gbuf=gbuf):
            yy, cc = y_line(line - q)
            cols = pl.ds(pl.multiple_of((yy * CORES + cc) * shard, shard), shard)
            remote(
                gbuf.at[0:thirds, :, cols], rs.at[g, c, y], rs_send.at[g], rs_recv.at[g],
                device(yy, cc, z, x),
            ).start()

        cols = pl.ds(pl.multiple_of((y * CORES + c) * shard, shard), shard)
        pltpu.make_async_copy(gbuf.at[0:thirds, :, cols], rs.at[g, c, y], rs_recv.at[g]).start()

    def shares(k, own, slots, metas, ret, send, got, out_hbm, weighted):
        def picks(m):
            hit0, hit1 = slots == m[0:1, :], slots == m[1:2, :]
            if not weighted:
                return [jnp.where(hit0 | hit1, 1.0, 0.0).astype(BF16)]
            g = jnp.where(hit0, m[2:3, :], 0.0) + jnp.where(hit1, m[3:4, :], 0.0)
            high = g.astype(BF16)
            return [high, (g - high.astype(F32)).astype(BF16)]

        @pl.loop(1, SIDE)
        def _(j):
            src = (own + step_of(j)) % SIDE
            await_bytes(ret.at[src], bwd_recv.at[k, src])
            weights = picks(metas[src])

            @pl.loop(0, SIDE)
            def _(n):
                cols = pl.ds(pl.multiple_of(n * tile, tile), tile)
                v = ret[src, :, cols]
                send[src, :, cols] = sum(dot(w, v, TN) for w in weights).astype(BF16)

            where = device(y, c, src, x) if k == 0 else device(y, c, z, src)
            slot = (own - src + SIDE - 1) % SIDE
            remote(send.at[src], got.at[slot], part_send.at[k, src], part_recv.at[k, slot], where).start()

    def finish(k, own, slots, metas, ret, send, got, out_hbm, weighted):
        await_bytes(ret.at[own], bwd_recv.at[k, own])
        m = metas[own]
        hit0, hit1 = slots == m[0:1, :], slots == m[1:2, :]
        if weighted:
            g = jnp.where(hit0, m[2:3, :], 0.0) + jnp.where(hit1, m[3:4, :], 0.0)
            high = g.astype(BF16)
            weights = [high, (g - high.astype(F32)).astype(BF16)]
        else:
            weights = [jnp.where(hit0 | hit1, 1.0, 0.0).astype(BF16)]

        @pl.loop(0, SIDE - 1)
        def _(slot):
            await_bytes(got.at[slot], part_recv.at[k, slot])

        @pl.loop(0, SIDE)
        def _(n):
            cols = pl.ds(pl.multiple_of(n * tile, tile), tile)
            v = ret[own, :, cols]
            total = sum(dot(w, v, TN) for w in weights)
            for slot in range(SIDE - 1):
                total = total + got[slot, :, cols].astype(F32)
            send[own, :, cols] = total.astype(BF16)

        pltpu.make_async_copy(send.at[own], out_hbm, out_sem.at[k]).start()

    fwd = (0, z, tok_slots, meta_z, ret_o, recv_t, pmr, mixed_hbm, True)
    bwd = (1, x, cot_slots, meta_x, ret_d, recv_c, pdr, igrad_hbm, False)
    shares(*fwd)
    shares(*bwd)
    finish(*fwd)

    await_bytes(rs.at[0], rs_recv.at[0])

    @pl.loop(0, CORES)
    def _(e):
        total = rs[0, e, 0].astype(F32)
        for yy in range(1, SIDE):
            total = total + rs[0, e, yy].astype(F32)
        gst[e] = total.reshape(hidden, shard)

    pltpu.make_async_copy(gst, dng_hbm, out_sem.at[2]).start()
    await_bytes(rs.at[1], rs_recv.at[1])

    @pl.loop(0, CORES)
    def _(e):
        total = rs[1, e, 0].astype(F32)
        for yy in range(1, SIDE):
            total = total + rs[1, e, yy].astype(F32)
        pre[e] = total.reshape(hidden, shard).T

    pltpu.make_async_copy(pre.at[0:CORES], upg_hbm, out_sem.at[3]).start()
    finish(*bwd)

    @pl.loop(0, SIDE)
    def _(j):
        for k, buf in ((0, sbuf_t), (1, sbuf_c)):
            await_bytes(buf.at[j, pl.ds(0, rows - cap)], bwd_send.at[k, j])

    @pl.loop(1, SIDE)
    def _(d):
        for k, own, buf in ((0, z, recv_t), (1, x, recv_c)):
            src = (own + d) % SIDE
            await_bytes(buf.at[src], part_send.at[k, src])

    for g, gbuf in ((0, cotbuf), (1, tokbuf)):
        await_bytes(gbuf.at[0:thirds, :, 0 : width - shard], rs_send.at[g])

    pltpu.make_async_copy(recv_t.at[z], mixed_hbm, out_sem.at[0]).wait()
    pltpu.make_async_copy(recv_c.at[x], igrad_hbm, out_sem.at[1]).wait()
    pltpu.make_async_copy(gst, dng_hbm, out_sem.at[2]).wait()
    pltpu.make_async_copy(pre.at[0:CORES], upg_hbm, out_sem.at[3]).wait()


def on_device(tokens, routes, gate_weights, w_up, w_down, cotangent):
    rows, width = tokens.shape
    held, _, hidden = w_up.shape
    shard = width // (SIDE * CORES)
    hbm = pl.BlockSpec(memory_space=pl.ANY)
    vmem = pl.BlockSpec(memory_space=pltpu.VMEM)
    four = pltpu.VMEM((SIDE, rows, width), BF16)
    three = pltpu.VMEM((SIDE - 1, rows, width), BF16)
    dma = pltpu.SemaphoreType.DMA
    mixed, igrad, upg, dng = pl.pallas_call(
        layer_kernel,
        out_shape=(
            jax.ShapeDtypeStruct((rows, width), BF16),
            jax.ShapeDtypeStruct((rows, width), BF16),
            jax.ShapeDtypeStruct((held, shard, hidden), F32),
            jax.ShapeDtypeStruct((held, hidden, shard), F32),
        ),
        in_specs=[hbm, hbm, vmem, vmem, hbm, hbm],
        out_specs=(hbm, hbm, hbm, hbm),
        scratch_shapes=[
            four, four,
            pltpu.VMEM((SIDE, 8, rows), F32), pltpu.VMEM((SIDE, 8, rows), F32),
            four, four, four, four,
            pltpu.VMEM((width, hidden), BF16), pltpu.VMEM((hidden, width), BF16),
            pltpu.VMEM((SIDE, rows, hidden), F32),
            pltpu.VMEM((SIDE, rows, hidden), BF16), pltpu.VMEM((SIDE, rows, hidden), BF16),
            four, four,
            pltpu.VMEM((2, CORES, SIDE, hidden // rows, rows, shard), BF16),
            three, three,
            pltpu.VMEM((CORES, hidden, shard), F32),
            dma((4,)), dma((2,)),
            dma((2, SIDE)), dma((2, SIDE)), dma((2, SIDE)), dma((2, SIDE)),
            dma((2, SIDE)), dma((2, SIDE)), dma((2, SIDE)), dma((2, SIDE)),
            dma((2,)), dma((2,)), dma((2, SIDE)), dma((2, SIDE)), dma((4,)),
        ],
        compiler_params=pltpu.CompilerParams(
            collective_id=0, has_side_effects=True, vmem_limit_bytes=63 << 20
        ),
    )(tokens, cotangent, routes.T, gate_weights.T, w_up, w_down)
    return (mixed, igrad, upg, dng)


def solution(mesh):
    rows = P(("dp", "expert"), None)
    held = P("expert", None, None)
    return jax.shard_map(
        on_device,
        mesh=mesh,
        in_specs=(rows, rows, rows, held, held, rows),
        out_specs=(rows, rows, P("expert", "dp", None), P("expert", None, "dp")),
        check_vma=False,
    )
```

```python
import jax
import jax.numpy as jnp
from jax import lax
from jax.experimental import pallas as pl
from jax.experimental.pallas import tpu as pltpu
from jax.sharding import PartitionSpec as P

MESH = pl.DeviceIdType.MESH
SIDE = 4
CORES = 2
F32 = jnp.float32
BF16 = jnp.bfloat16


def dot(a, b, dims):
    return lax.dot_general(a, b, (dims, ((), ())), preferred_element_type=F32)


NN = ((1,), (0,))
NT = ((1,), (1,))
TN = ((0,), (0,))


def sigmoid(v):
    return 1.0 / (1.0 + jnp.exp(-v))


def step_of(j):
    return j ^ (j // 2)


def layer_kernel(
    tok_hbm, cot_hbm, routes, gates, wup_hbm, wdn_hbm,
    mixed_hbm, igrad_hbm, upg_hbm, dng_hbm,
    tokbuf, cotbuf, meta_z, meta_x, sbuf_t, sbuf_c, recv_t, recv_c, wu, wd,
    pre, act, dpre, ret_o, ret_d, rs, pmr, pdr, gst,
    load_sem, ag_send, ag_recv, hand_send, meta_send, meta_recv,
    fwd_send, fwd_recv, bwd_send, bwd_recv, rs_send, rs_recv, part_send, part_recv, out_sem,
):
    dp, ex = lax.axis_index("dp"), lax.axis_index("expert")
    y, c = dp // CORES, dp % CORES
    z, x = ex // SIDE, ex % SIDE
    rows, width = tok_hbm.shape
    hidden = wup_hbm.shape[2]
    cap = rows // (SIDE * CORES)
    pair = CORES * cap
    tile = width // SIDE
    shard = width // (SIDE * CORES)
    line = SIDE * CORES
    mine = (x * CORES + c) * cap
    mine_z = (z * CORES + c) * cap

    def device(yy, cc, zz, xx):
        return (yy * CORES + cc, zz * SIDE + xx)

    def x_line(q):
        return (x + q // CORES) % SIDE, (c + q % CORES) % CORES

    def z_line(q):
        return (z + q // CORES) % SIDE, (c + q % CORES) % CORES

    def y_line(q):
        return (y + q // CORES) % SIDE, (c + q % CORES) % CORES

    def remote(src, dst, ssem, rsem, where):
        return pltpu.make_async_remote_copy(
            src_ref=src, dst_ref=dst, send_sem=ssem, recv_sem=rsem,
            device_id=where, device_id_type=MESH,
        )

    half = rows // 2
    halves = (pl.ds(0, half), pl.ds(half, half))

    def near(k, d):
        if k == 0:
            return device(y, c, (z + d) % SIDE, x)
        return device(y, c, z, (x + d) % SIDE)

    def await_bytes(ref, sem):
        pltpu.make_async_copy(ref, ref, sem).wait()

    tok_in = pltpu.make_async_copy(tok_hbm, tokbuf.at[z], load_sem.at[0])
    cot_in = pltpu.make_async_copy(cot_hbm, cotbuf.at[x], load_sem.at[1])
    wup_in = pltpu.make_async_copy(wup_hbm.at[c], wu, load_sem.at[2])
    wdn_in = pltpu.make_async_copy(wdn_hbm.at[c], wd, load_sem.at[3])
    tok_in.start()
    cot_in.start()

    barrier = pltpu.get_barrier_semaphore()

    def greet(where):
        pl.semaphore_signal(barrier, inc=1, device_id=where, device_id_type=MESH)

    @pl.loop(1, line)
    def _(q):
        xx, cc = x_line(q)
        greet(device(y, cc, z, xx))

    @pl.loop(CORES, line)
    def _(q):
        zz, cc = z_line(q)
        greet(device(y, cc, zz, x))
        yy, cc = y_line(q)
        greet(device(yy, cc, z, x))

    r0, r1 = routes[0:1, :], routes[1:2, :]
    experts = line * SIDE
    names = lax.broadcasted_iota(jnp.int32, (experts, rows), 0)
    hit0, hit1 = names == r0, names == r1
    onehot = jnp.where(hit0 | hit1, 1.0, 0.0).astype(BF16)
    earlier = (
        lax.broadcasted_iota(jnp.int32, (rows, rows), 0)
        < lax.broadcasted_iota(jnp.int32, (rows, rows), 1)
    )
    before = dot(onehot, jnp.where(earlier, 1.0, 0.0).astype(BF16), NN)
    slot0 = r0.astype(F32) * cap + jnp.sum(jnp.where(hit0, before, 0.0), axis=0, keepdims=True)
    slot1 = r1.astype(F32) * cap + jnp.sum(jnp.where(hit1, before, 0.0), axis=0, keepdims=True)
    meta = jnp.concatenate(
        [slot0, slot1, gates[0:1, :], gates[1:2, :], jnp.zeros((4, rows), F32)], axis=0
    )
    meta_z[z] = meta
    meta_x[x] = meta

    pl.semaphore_wait(barrier, line - 1 + 2 * (line - CORES))

    @pl.loop(1, SIDE)
    def _(j):
        d = step_of(j)
        to_z, to_x = device(y, c, (z + d) % SIDE, x), device(y, c, z, (x + d) % SIDE)
        remote(meta_z.at[z], meta_z.at[z], meta_send.at[0, d], meta_recv.at[0, z], to_z).start()
        remote(meta_x.at[x], meta_x.at[x], meta_send.at[1, d], meta_recv.at[1, x], to_x).start()

    tok_in.wait()
    cot_in.wait()

    axes = ((0, tokbuf, z), (1, cotbuf, x))
    for first in (True, False):
        for k, buf, own in axes:
            for side, d in ((0, 1), (1, SIDE - 1)):
                h = side if first else 1 - side
                part = buf.at[own, halves[h]]
                remote(part, part, ag_send.at[k, side, h], ag_recv.at[k, own, h], near(k, d)).start()

    wup_in.start()
    wdn_in.start()

    place = lax.broadcasted_iota(jnp.int32, (rows, rows), 0)
    tok_slots = (place + z * rows).astype(F32)
    cot_slots = ((place // pair) * rows + x * pair + place % pair).astype(F32)

    @pl.loop(0, SIDE)
    def _(j):
        d = step_of(j)
        zs, xs = (z + d) % SIDE, (x + d) % SIDE

        @pl.when(j == 1)
        def _():
            for k, buf, own in axes:
                for side, back, ahead in ((0, SIDE - 1, 1), (1, 1, SIDE - 1)):
                    src = (own + back) % SIDE
                    part = buf.at[src, halves[side]]
                    await_bytes(part, ag_recv.at[k, src, side])
                    remote(part, part, hand_send.at[k, side], ag_recv.at[k, src, side], near(k, ahead)).start()

        def arrived(k, buf, metas, src):
            @pl.when(j > 0)
            def _():
                await_bytes(metas.at[src], meta_recv.at[k, src])

            @pl.when((d == 1) | (d == 2))
            def _():
                await_bytes(buf.at[src, halves[0]], ag_recv.at[k, src, 0])

            @pl.when((d == SIDE - 1) | (d == 2))
            def _():
                await_bytes(buf.at[src, halves[1]], ag_recv.at[k, src, 1])

        arrived(0, tokbuf, meta_z, zs)
        m = meta_z[zs]
        pick = jnp.where((tok_slots == m[0:1, :]) | (tok_slots == m[1:2, :]), 1.0, 0.0).astype(BF16)

        @pl.loop(0, SIDE)
        def _(n):
            cols = pl.ds(pl.multiple_of(n * tile, tile), tile)
            sbuf_t[zs, :, cols] = dot(pick, tokbuf[zs, :, cols], NN).astype(BF16)

        @pl.loop(1, line)
        def _(q):
            xx, cc = x_line(q)
            remote(
                sbuf_t.at[zs, pl.ds((xx * CORES + cc) * cap, cap)],
                recv_t.at[zs, pl.ds(mine, cap)],
                fwd_send.at[0, zs], fwd_recv.at[0, zs], device(y, cc, z, xx),
            ).start()

        pltpu.make_async_copy(
            sbuf_t.at[zs, pl.ds(mine, cap)], recv_t.at[zs, pl.ds(mine, cap)], fwd_recv.at[0, zs]
        ).start()

        arrived(1, cotbuf, meta_x, xs)
        m = meta_x[xs]
        hit0, hit1 = cot_slots == m[0:1, :], cot_slots == m[1:2, :]
        pick = jnp.where(hit0 | hit1, 1.0, 0.0).astype(BF16)
        scale = jnp.sum(
            jnp.where(hit0, m[2:3, :], 0.0) + jnp.where(hit1, m[3:4, :], 0.0), axis=1, keepdims=True
        )

        @pl.loop(0, SIDE)
        def _(n):
            cols = pl.ds(pl.multiple_of(n * tile, tile), tile)
            sbuf_c[xs, :, cols] = (dot(pick, cotbuf[xs, :, cols], NN) * scale).astype(BF16)

        @pl.loop(1, line)
        def _(q):
            zz, cc = z_line(q)
            remote(
                sbuf_c.at[xs, pl.ds((zz * CORES + cc) * cap, cap)],
                recv_c.at[z, pl.ds((xs * CORES + c) * cap, cap)],
                fwd_send.at[1, xs], fwd_recv.at[1, xs], device(y, cc, zz, x),
            ).start()

        pltpu.make_async_copy(
            sbuf_c.at[xs, pl.ds(mine_z, cap)],
            recv_c.at[z, pl.ds((xs * CORES + c) * cap, cap)],
            fwd_recv.at[1, xs],
        ).start()

    wup_in.wait()
    wdn_in.wait()

    @pl.loop(0, SIDE)
    def _(j):
        zs = (z + step_of(j)) % SIDE
        await_bytes(recv_t.at[zs], fwd_recv.at[0, zs])
        v = dot(recv_t[zs], wu[...], NN)
        pre[zs] = v
        a = (v * sigmoid(v)).astype(BF16)
        act[zs] = a
        await_bytes(sbuf_t.at[zs, pl.ds(0, rows - cap)], fwd_send.at[0, zs])

        @pl.loop(0, SIDE)
        def _(n):
            cols = pl.ds(pl.multiple_of(n * tile, tile), tile)
            sbuf_t[zs, :, cols] = dot(act[zs], wd[:, cols], NN).astype(BF16)

        @pl.loop(1, line)
        def _(q):
            xx, cc = x_line(q)
            remote(
                sbuf_t.at[zs, pl.ds((xx * CORES + cc) * cap, cap)],
                ret_o.at[zs, pl.ds(mine, cap)],
                bwd_send.at[0, zs], bwd_recv.at[0, zs], device(y, cc, z, xx),
            ).start()

        pltpu.make_async_copy(
            sbuf_t.at[zs, pl.ds(mine, cap)], ret_o.at[zs, pl.ds(mine, cap)], bwd_recv.at[0, zs]
        ).start()

    @pl.loop(0, SIDE)
    def _(j):
        xs = (x + step_of(j)) % SIDE
        part = pl.ds(pl.multiple_of(xs * pair, pair), pair)
        await_bytes(recv_c.at[:, part], fwd_recv.at[1, xs])
        da = dot(recv_c[:, part, :].reshape(rows, width), wd[...], NT)
        v = pre[:, part, :].reshape(rows, hidden)
        s = sigmoid(v)
        dp_rows = (da * s * (1.0 + v * (1.0 - s))).astype(BF16)
        dpre[:, part, :] = dp_rows.reshape(SIDE, pair, hidden)
        await_bytes(sbuf_c.at[xs, pl.ds(0, rows - cap)], fwd_send.at[1, xs])

        @pl.loop(0, SIDE)
        def _(n):
            cols = pl.ds(pl.multiple_of(n * tile, tile), tile)
            left = dpre[:, part, :].reshape(rows, hidden)
            sbuf_c[xs, :, cols] = dot(left, wu[cols, :], NT).astype(BF16)

        @pl.loop(1, line)
        def _(q):
            zz, cc = z_line(q)
            remote(
                sbuf_c.at[xs, pl.ds((zz * CORES + cc) * cap, cap)],
                ret_d.at[xs, pl.ds(mine_z, cap)],
                bwd_send.at[1, xs], bwd_recv.at[1, xs], device(y, cc, zz, x),
            ).start()

        pltpu.make_async_copy(
            sbuf_c.at[xs, pl.ds(mine_z, cap)], ret_d.at[xs, pl.ds(mine_z, cap)], bwd_recv.at[1, xs]
        ).start()

    @pl.loop(1, SIDE)
    def _(d):
        for k, own, metas in ((0, z, meta_z), (1, x, meta_x)):
            await_bytes(metas.at[own], meta_send.at[k, d])

    for k, buf, own in axes:
        for side, back in ((0, SIDE - 1), (1, 1)):
            for h in range(2):
                await_bytes(buf.at[own, halves[h]], ag_send.at[k, side, h])
            await_bytes(buf.at[(own + back) % SIDE, halves[side]], hand_send.at[k, side])

    thirds = hidden // rows
    for g, left, right, gbuf in ((0, act, recv_c, cotbuf), (1, dpre, recv_t, tokbuf)):

        @pl.loop(0, SIDE)
        def _(n, g=g, left=left, right=right, gbuf=gbuf):
            yy = (y + step_of(SIDE - 1 - n)) % SIDE
            cols = pl.ds(pl.multiple_of(yy * tile, tile), tile)
            r = dot(
                left[...].reshape(SIDE * rows, hidden),
                right[:, :, cols].reshape(SIDE * rows, tile),
                TN,
            )
            gbuf[0:thirds, :, cols] = r.astype(BF16).reshape(thirds, rows, tile)

        @pl.loop(1, line)
        def _(q, g=g, gbuf=gbuf):
            yy, cc = y_line(line - q)
            cols = pl.ds(pl.multiple_of((yy * CORES + cc) * shard, shard), shard)
            remote(
                gbuf.at[0:thirds, :, cols], rs.at[g, c, y], rs_send.at[g], rs_recv.at[g],
                device(yy, cc, z, x),
            ).start()

        cols = pl.ds(pl.multiple_of((y * CORES + c) * shard, shard), shard)
        pltpu.make_async_copy(gbuf.at[0:thirds, :, cols], rs.at[g, c, y], rs_recv.at[g]).start()

    def share(k, own, slots, metas, ret, weighted):
        def of(src, h, cols):
            m = metas[src]
            m = m[:, h * half : (h + 1) * half]
            hit0, hit1 = slots[:, 0:half] == m[0:1, :], slots[:, 0:half] == m[1:2, :]
            v = ret[src, :, cols]
            if not weighted:
                return dot(jnp.where(hit0 | hit1, 1.0, 0.0).astype(BF16), v, TN)
            g = jnp.where(hit0, m[2:3, :], 0.0) + jnp.where(hit1, m[3:4, :], 0.0)
            high = g.astype(BF16)
            low = (g - high.astype(F32)).astype(BF16)
            return dot(high, v, TN) + dot(low, v, TN)
        return of

    def tiles(body):
        @pl.loop(0, SIDE)
        def _(n):
            body(pl.ds(pl.multiple_of(n * tile, tile), tile))

    def pass_on(k, send, got, src, h, slot, where_d):
        part = send.at[src, halves[h]]
        remote(part, got.at[slot, halves[h]], part_send.at[k, slot, h], part_recv.at[k, slot, h], near(k, where_d)).start()

    def shares(k, own, slots, metas, ret, send, got, out_hbm, weighted):
        of = share(k, own, slots, metas, ret, weighted)
        ahead, behind, far = (own + 1) % SIDE, (own + SIDE - 1) % SIDE, (own + 2) % SIDE
        for src, h, slot, d in ((ahead, 1, 1, 1), (behind, 0, 0, SIDE - 1)):
            await_bytes(ret.at[src], bwd_recv.at[k, src])

            def body(cols, src=src, h=h):
                send[src, halves[h], cols] = of(src, h, cols).astype(BF16)

            tiles(body)
            pass_on(k, send, got, src, h, slot, d)
        await_bytes(ret.at[far], bwd_recv.at[k, far])
        for h, d in ((0, 1), (1, SIDE - 1)):
            def body(cols, h=h):
                send[far, halves[h], cols] = of(far, h, cols).astype(BF16)

            tiles(body)
            pass_on(k, send, got, far, h, 2, d)

    def hand_on(k, own, slots, metas, ret, send, got, out_hbm, weighted):
        of = share(k, own, slots, metas, ret, weighted)
        ahead, behind = (own + 1) % SIDE, (own + SIDE - 1) % SIDE
        for src, h, slot, d in ((ahead, 0, 1, 1), (behind, 1, 0, SIDE - 1)):
            await_bytes(got.at[2, halves[h]], part_recv.at[k, 2, h])

            def body(cols, src=src, h=h):
                total = of(src, h, cols) + got[2, halves[h], cols].astype(F32)
                send[src, halves[h], cols] = total.astype(BF16)

            tiles(body)
            pass_on(k, send, got, src, h, slot, d)

    def finish(k, own, slots, metas, ret, send, got, out_hbm, weighted):
        of = share(k, own, slots, metas, ret, weighted)
        await_bytes(ret.at[own], bwd_recv.at[k, own])
        for slot in range(2):
            for h in range(2):
                await_bytes(got.at[slot, halves[h]], part_recv.at[k, slot, h])
        for h in range(2):
            def body(cols, h=h):
                total = of(own, h, cols) + got[0, halves[h], cols].astype(F32)
                send[own, halves[h], cols] = (total + got[1, halves[h], cols].astype(F32)).astype(BF16)

            tiles(body)
        pltpu.make_async_copy(send.at[own], out_hbm, out_sem.at[k]).start()

    fwd = (0, z, tok_slots, meta_z, ret_o, recv_t, pmr, mixed_hbm, True)
    bwd = (1, x, cot_slots, meta_x, ret_d, recv_c, pdr, igrad_hbm, False)
    shares(*fwd)
    shares(*bwd)
    hand_on(*fwd)
    hand_on(*bwd)
    finish(*fwd)

    await_bytes(rs.at[0], rs_recv.at[0])

    @pl.loop(0, CORES)
    def _(e):
        total = rs[0, e, 0].astype(F32)
        for yy in range(1, SIDE):
            total = total + rs[0, e, yy].astype(F32)
        gst[e] = total.reshape(hidden, shard)

    pltpu.make_async_copy(gst, dng_hbm, out_sem.at[2]).start()
    await_bytes(rs.at[1], rs_recv.at[1])

    @pl.loop(0, CORES)
    def _(e):
        total = rs[1, e, 0].astype(F32)
        for yy in range(1, SIDE):
            total = total + rs[1, e, yy].astype(F32)
        pre[e] = total.reshape(hidden, shard).T

    pltpu.make_async_copy(pre.at[0:CORES], upg_hbm, out_sem.at[3]).start()
    finish(*bwd)

    @pl.loop(0, SIDE)
    def _(j):
        for k, buf in ((0, sbuf_t), (1, sbuf_c)):
            await_bytes(buf.at[j, pl.ds(0, rows - cap)], bwd_send.at[k, j])

    for k, got in ((0, pmr), (1, pdr)):
        for slot in range(SIDE - 1):
            for h in range(2):
                await_bytes(got.at[slot, halves[h]], part_send.at[k, slot, h])

    for g, gbuf in ((0, cotbuf), (1, tokbuf)):
        await_bytes(gbuf.at[0:thirds, :, 0 : width - shard], rs_send.at[g])

    pltpu.make_async_copy(recv_t.at[z], mixed_hbm, out_sem.at[0]).wait()
    pltpu.make_async_copy(recv_c.at[x], igrad_hbm, out_sem.at[1]).wait()
    pltpu.make_async_copy(gst, dng_hbm, out_sem.at[2]).wait()
    pltpu.make_async_copy(pre.at[0:CORES], upg_hbm, out_sem.at[3]).wait()


def copy_kernel(*refs):
    srcs, dsts, bufs, sem = refs[0:4], refs[4:8], refs[8:12], refs[12]
    pieces = []
    for i in range(4):
        first = srcs[i].shape[0] // 2
        pieces += [(i, h, pl.ds(h * first, first)) for h in range(2)]
    for i, h, part in pieces:
        pltpu.make_async_copy(srcs[i].at[part], bufs[i].at[part], sem.at[0, i, h]).start()
    for i, h, part in pieces:
        pltpu.make_async_copy(srcs[i].at[part], bufs[i].at[part], sem.at[0, i, h]).wait()
        pltpu.make_async_copy(bufs[i].at[part], dsts[i].at[part], sem.at[1, i, h]).start()
    for i, h, part in pieces:
        pltpu.make_async_copy(bufs[i].at[part], dsts[i].at[part], sem.at[1, i, h]).wait()


def on_device(tokens, routes, gate_weights, w_up, w_down, cotangent):
    rows, width = tokens.shape
    held, _, hidden = w_up.shape
    shard = width // (SIDE * CORES)
    hbm = pl.BlockSpec(memory_space=pl.ANY)
    vmem = pl.BlockSpec(memory_space=pltpu.VMEM)
    four = pltpu.VMEM((SIDE, rows, width), BF16)
    three = pltpu.VMEM((SIDE - 1, rows, width), BF16)
    dma = pltpu.SemaphoreType.DMA
    results = pl.pallas_call(
        layer_kernel,
        out_shape=(
            jax.ShapeDtypeStruct((rows, width), BF16),
            jax.ShapeDtypeStruct((rows, width), BF16),
            jax.ShapeDtypeStruct((held, shard, hidden), F32),
            jax.ShapeDtypeStruct((held, hidden, shard), F32),
        ),
        in_specs=[hbm, hbm, vmem, vmem, hbm, hbm],
        out_specs=(hbm, hbm, hbm, hbm),
        scratch_shapes=[
            four, four,
            pltpu.VMEM((SIDE, 8, rows), F32), pltpu.VMEM((SIDE, 8, rows), F32),
            four, four, four, four,
            pltpu.VMEM((width, hidden), BF16), pltpu.VMEM((hidden, width), BF16),
            pltpu.VMEM((SIDE, rows, hidden), F32),
            pltpu.VMEM((SIDE, rows, hidden), BF16), pltpu.VMEM((SIDE, rows, hidden), BF16),
            four, four,
            pltpu.VMEM((2, CORES, SIDE, hidden // rows, rows, shard), BF16),
            three, three,
            pltpu.VMEM((CORES, hidden, shard), F32),
            dma((4,)), dma((2, 2, 2)), dma((2, SIDE, 2)), dma((2, 2)),
            dma((2, SIDE)), dma((2, SIDE)),
            dma((2, SIDE)), dma((2, SIDE)), dma((2, SIDE)), dma((2, SIDE)),
            dma((2,)), dma((2,)), dma((2, SIDE - 1, 2)), dma((2, SIDE - 1, 2)), dma((4,)),
        ],
        compiler_params=pltpu.CompilerParams(
            collective_id=0, has_side_effects=True, vmem_limit_bytes=63 << 20
        ),
    )(tokens, cotangent, routes.T, gate_weights.T, w_up, w_down)
    return pl.pallas_call(
        copy_kernel,
        out_shape=tuple(jax.ShapeDtypeStruct(r.shape, r.dtype) for r in results),
        in_specs=[hbm] * 4,
        out_specs=(hbm,) * 4,
        scratch_shapes=[pltpu.VMEM(r.shape, r.dtype) for r in results] + [dma((2, 4, 2))],
    )(*results)


def solution(mesh):
    rows = P(("dp", "expert"), None)
    held = P("expert", None, None)
    return jax.shard_map(
        on_device,
        mesh=mesh,
        in_specs=(rows, rows, rows, held, held, rows),
        out_specs=(rows, rows, P("expert", "dp", None), P("expert", None, "dp")),
        check_vma=False,
    )
```

```python
import jax
import jax.numpy as jnp
from jax import lax
from jax.experimental import pallas as pl
from jax.experimental.pallas import tpu as pltpu
from jax.sharding import PartitionSpec as P

MESH = pl.DeviceIdType.MESH
SIDE = 4
CORES = 2
F32 = jnp.float32
BF16 = jnp.bfloat16


def dot(a, b, dims):
    return lax.dot_general(a, b, (dims, ((), ())), preferred_element_type=F32)


NN = ((1,), (0,))
NT = ((1,), (1,))
TN = ((0,), (0,))


def sigmoid(v):
    return 1.0 / (1.0 + jnp.exp(-v))


def step_of(j):
    return j ^ (j // 2)


def layer_kernel(
    tok_hbm, cot_hbm, routes, gates, wup_hbm, wdn_hbm,
    mixed_hbm, igrad_hbm, upg_hbm, dng_hbm,
    tokbuf, cotbuf, meta_z, meta_x, sbuf_t, sbuf_c, recv_t, recv_c, wu, wd,
    pre, act, dpre, ret_o, ret_d, rs, pmr, pdr, gst,
    load_sem, ag_send, ag_recv, hand_send, meta_send, meta_recv, fwd_own,
    fwd_send, fwd_recv, bwd_send, bwd_recv, rs_send, rs_recv, part_send, part_recv, out_sem,
):
    dp, ex = lax.axis_index("dp"), lax.axis_index("expert")
    y, c = dp // CORES, dp % CORES
    z, x = ex // SIDE, ex % SIDE
    rows, width = tok_hbm.shape
    hidden = wup_hbm.shape[2]
    cap = rows // (SIDE * CORES)
    pair = CORES * cap
    tile = width // SIDE
    shard = width // (SIDE * CORES)
    line = SIDE * CORES
    mine = (x * CORES + c) * cap
    mine_z = (z * CORES + c) * cap

    def device(yy, cc, zz, xx):
        return (yy * CORES + cc, zz * SIDE + xx)

    def x_line(q):
        return (x + q // CORES) % SIDE, (c + q % CORES) % CORES

    def z_line(q):
        return (z + q // CORES) % SIDE, (c + q % CORES) % CORES

    def y_line(q):
        return (y + q // CORES) % SIDE, (c + q % CORES) % CORES

    def remote(src, dst, ssem, rsem, where):
        return pltpu.make_async_remote_copy(
            src_ref=src, dst_ref=dst, send_sem=ssem, recv_sem=rsem,
            device_id=where, device_id_type=MESH,
        )

    half = rows // 2
    halves = (pl.ds(0, half), pl.ds(half, half))

    def near(k, d):
        if k == 0:
            return device(y, c, (z + d) % SIDE, x)
        return device(y, c, z, (x + d) % SIDE)

    def await_bytes(ref, sem):
        pltpu.make_async_copy(ref, ref, sem).wait()

    tok_in = pltpu.make_async_copy(tok_hbm, tokbuf.at[z], load_sem.at[0])
    cot_in = pltpu.make_async_copy(cot_hbm, cotbuf.at[x], load_sem.at[1])
    wup_in = pltpu.make_async_copy(wup_hbm.at[c], wu, load_sem.at[2])
    wdn_in = pltpu.make_async_copy(wdn_hbm.at[c], wd, load_sem.at[3])
    tok_in.start()
    cot_in.start()

    barrier = pltpu.get_barrier_semaphore()

    def greet(where):
        pl.semaphore_signal(barrier, inc=1, device_id=where, device_id_type=MESH)

    @pl.loop(1, line)
    def _(q):
        xx, cc = x_line(q)
        greet(device(y, cc, z, xx))

    @pl.loop(CORES, line)
    def _(q):
        zz, cc = z_line(q)
        greet(device(y, cc, zz, x))
        yy, cc = y_line(q)
        greet(device(yy, cc, z, x))

    r0, r1 = routes[0:1, :], routes[1:2, :]
    experts = line * SIDE
    names = lax.broadcasted_iota(jnp.int32, (experts, rows), 0)
    hit0, hit1 = names == r0, names == r1
    onehot = jnp.where(hit0 | hit1, 1.0, 0.0).astype(BF16)
    earlier = (
        lax.broadcasted_iota(jnp.int32, (rows, rows), 0)
        < lax.broadcasted_iota(jnp.int32, (rows, rows), 1)
    )
    before = dot(onehot, jnp.where(earlier, 1.0, 0.0).astype(BF16), NN)
    slot0 = r0.astype(F32) * cap + jnp.sum(jnp.where(hit0, before, 0.0), axis=0, keepdims=True)
    slot1 = r1.astype(F32) * cap + jnp.sum(jnp.where(hit1, before, 0.0), axis=0, keepdims=True)
    meta = jnp.concatenate(
        [slot0, slot1, gates[0:1, :], gates[1:2, :], jnp.zeros((4, rows), F32)], axis=0
    )
    meta_z[z] = meta
    meta_x[x] = meta

    pl.semaphore_wait(barrier, line - 1 + 2 * (line - CORES))

    @pl.loop(1, SIDE)
    def _(j):
        d = step_of(j)
        to_z, to_x = device(y, c, (z + d) % SIDE, x), device(y, c, z, (x + d) % SIDE)
        remote(meta_z.at[z], meta_z.at[z], meta_send.at[0, d], meta_recv.at[0, z], to_z).start()
        remote(meta_x.at[x], meta_x.at[x], meta_send.at[1, d], meta_recv.at[1, x], to_x).start()

    tok_in.wait()
    cot_in.wait()

    axes = ((0, tokbuf, z), (1, cotbuf, x))
    for first in (True, False):
        for k, buf, own in axes:
            for side, d in ((0, 1), (1, SIDE - 1)):
                h = side if first else 1 - side
                part = buf.at[own, halves[h]]
                remote(part, part, ag_send.at[k, side, h], ag_recv.at[k, own, h], near(k, d)).start()

    wup_in.start()
    wdn_in.start()

    place = lax.broadcasted_iota(jnp.int32, (rows, rows), 0)
    tok_slots = (place + z * rows).astype(F32)
    cot_slots = ((place // pair) * rows + x * pair + place % pair).astype(F32)

    def tiles(body):
        @pl.loop(0, SIDE)
        def _(n):
            body(pl.ds(pl.multiple_of(n * tile, tile), tile))

    def hand_over():
        for k, buf, own in axes:
            for side, back, ahead in ((0, SIDE - 1, 1), (1, 1, SIDE - 1)):
                src = (own + back) % SIDE
                part = buf.at[src, halves[side]]
                await_bytes(part, ag_recv.at[k, src, side])
                remote(part, part, hand_send.at[k, side], ag_recv.at[k, src, side], near(k, ahead)).start()

    def arrived(k, buf, metas, src, d):
        if d != 0:
            await_bytes(metas.at[src], meta_recv.at[k, src])
        if d in (1, 2):
            await_bytes(buf.at[src, halves[0]], ag_recv.at[k, src, 0])
        if d in (SIDE - 1, 2):
            await_bytes(buf.at[src, halves[1]], ag_recv.at[k, src, 1])

    def relay_tokens(d):
        zs = (z + d) % SIDE
        arrived(0, tokbuf, meta_z, zs, d)
        m = meta_z[zs]
        pick = jnp.where((tok_slots == m[0:1, :]) | (tok_slots == m[1:2, :]), 1.0, 0.0).astype(BF16)

        def body(cols):
            sbuf_t[zs, :, cols] = dot(pick, tokbuf[zs, :, cols], NN).astype(BF16)

        tiles(body)

        def send(q, sem):
            xx, cc = x_line(q)
            remote(
                sbuf_t.at[zs, pl.ds((xx * CORES + cc) * cap, cap)],
                recv_t.at[zs, pl.ds(mine, cap)],
                fwd_send.at[0, zs], sem, device(y, cc, z, xx),
            ).start()

        send(1, fwd_own.at[zs])
        pltpu.make_async_copy(
            sbuf_t.at[zs, pl.ds(mine, cap)], recv_t.at[zs, pl.ds(mine, cap)], fwd_own.at[zs]
        ).start()

        @pl.loop(CORES, line)
        def _(q):
            send(q, fwd_recv.at[0, zs])

    def relay_cotangents(d):
        xs = (x + d) % SIDE
        arrived(1, cotbuf, meta_x, xs, d)
        m = meta_x[xs]
        hit0, hit1 = cot_slots == m[0:1, :], cot_slots == m[1:2, :]
        pick = jnp.where(hit0 | hit1, 1.0, 0.0).astype(BF16)
        scale = jnp.sum(
            jnp.where(hit0, m[2:3, :], 0.0) + jnp.where(hit1, m[3:4, :], 0.0), axis=1, keepdims=True
        )

        def body(cols):
            sbuf_c[xs, :, cols] = (dot(pick, cotbuf[xs, :, cols], NN) * scale).astype(BF16)

        tiles(body)

        @pl.loop(1, line)
        def _(q):
            zz, cc = z_line(q)
            remote(
                sbuf_c.at[xs, pl.ds((zz * CORES + cc) * cap, cap)],
                recv_c.at[z, pl.ds((xs * CORES + c) * cap, cap)],
                fwd_send.at[1, xs], fwd_recv.at[1, xs], device(y, cc, zz, x),
            ).start()

        pltpu.make_async_copy(
            sbuf_c.at[xs, pl.ds(mine_z, cap)],
            recv_c.at[z, pl.ds((xs * CORES + c) * cap, cap)],
            fwd_recv.at[1, xs],
        ).start()

    def column(xs):
        return pl.ds(pl.multiple_of(xs * pair, pair), pair)

    def activate_column():
        for d in range(SIDE):
            zs = (z + d) % SIDE
            await_bytes(recv_t.at[zs, column(x)], fwd_own.at[zs])
        v = dot(recv_t[:, column(x), :].reshape(SIDE * pair, width), wu[...], NN)
        pre[:, column(x), :] = v.reshape(SIDE, pair, hidden)

    def forward(d):
        zs = (z + d) % SIDE
        await_bytes(recv_t.at[zs, 0 : rows - pair], fwd_recv.at[0, zs])
        v = dot(recv_t[zs], wu[...], NN)
        pre[zs] = v
        act[zs] = (v * sigmoid(v)).astype(BF16)
        await_bytes(sbuf_t.at[zs, pl.ds(0, rows - cap)], fwd_send.at[0, zs])

        def body(cols):
            sbuf_t[zs, :, cols] = dot(act[zs], wd[:, cols], NN).astype(BF16)

        tiles(body)

        @pl.loop(1, line)
        def _(q):
            xx, cc = x_line(q)
            remote(
                sbuf_t.at[zs, pl.ds((xx * CORES + cc) * cap, cap)],
                ret_o.at[zs, pl.ds(mine, cap)],
                bwd_send.at[0, zs], bwd_recv.at[0, zs], device(y, cc, z, xx),
            ).start()

        pltpu.make_async_copy(
            sbuf_t.at[zs, pl.ds(mine, cap)], ret_o.at[zs, pl.ds(mine, cap)], bwd_recv.at[0, zs]
        ).start()

    def cotangents_in(d):
        xs = (x + d) % SIDE
        await_bytes(recv_c.at[:, column(xs)], fwd_recv.at[1, xs])

    def backward(d):
        xs = (x + d) % SIDE
        part = column(xs)
        da = dot(recv_c[:, part, :].reshape(rows, width), wd[...], NT)
        v = pre[:, part, :].reshape(rows, hidden)
        s = sigmoid(v)
        dp_rows = (da * s * (1.0 + v * (1.0 - s))).astype(BF16)
        dpre[:, part, :] = dp_rows.reshape(SIDE, pair, hidden)
        await_bytes(sbuf_c.at[xs, pl.ds(0, rows - cap)], fwd_send.at[1, xs])

        def body(cols):
            left = dpre[:, part, :].reshape(rows, hidden)
            sbuf_c[xs, :, cols] = dot(left, wu[cols, :], NT).astype(BF16)

        tiles(body)

        @pl.loop(1, line)
        def _(q):
            zz, cc = z_line(q)
            remote(
                sbuf_c.at[xs, pl.ds((zz * CORES + cc) * cap, cap)],
                ret_d.at[xs, pl.ds(mine_z, cap)],
                bwd_send.at[1, xs], bwd_recv.at[1, xs], device(y, cc, zz, x),
            ).start()

        pltpu.make_async_copy(
            sbuf_c.at[xs, pl.ds(mine_z, cap)], ret_d.at[xs, pl.ds(mine_z, cap)], bwd_recv.at[1, xs]
        ).start()

    def drain():
        @pl.loop(1, SIDE)
        def _(d):
            for k, own, metas in ((0, z, meta_z), (1, x, meta_x)):
                await_bytes(metas.at[own], meta_send.at[k, d])

        for k, buf, own in axes:
            for side, back in ((0, SIDE - 1), (1, 1)):
                for h in range(2):
                    await_bytes(buf.at[own, halves[h]], ag_send.at[k, side, h])
                await_bytes(buf.at[(own + back) % SIDE, halves[side]], hand_send.at[k, side])

    thirds = hidden // rows

    def weight_grad(g):
        left, right, gbuf = ((act, recv_c, cotbuf), (dpre, recv_t, tokbuf))[g]

        def body(cols):
            r = dot(
                left[...].reshape(SIDE * rows, hidden),
                right[:, :, cols].reshape(SIDE * rows, tile),
                TN,
            )
            gbuf[0:thirds, :, cols] = r.astype(BF16).reshape(thirds, rows, tile)

        tiles(body)

        @pl.loop(1, line)
        def _(q):
            yy, cc = y_line(q)
            cols = pl.ds(pl.multiple_of((yy * CORES + cc) * shard, shard), shard)
            remote(
                gbuf.at[0:thirds, :, cols], rs.at[g, c, y], rs_send.at[g], rs_recv.at[g],
                device(yy, cc, z, x),
            ).start()

        cols = pl.ds(pl.multiple_of((y * CORES + c) * shard, shard), shard)
        pltpu.make_async_copy(gbuf.at[0:thirds, :, cols], rs.at[g, c, y], rs_recv.at[g]).start()

    def gradients_out(g):
        await_bytes(rs.at[g], rs_recv.at[g])

        @pl.loop(0, CORES)
        def _(e):
            total = rs[g, e, 0].astype(F32)
            for yy in range(1, SIDE):
                total = total + rs[g, e, yy].astype(F32)
            if g == 0:
                gst[e] = total.reshape(hidden, shard)
            else:
                pre[e] = total.reshape(hidden, shard).T

        if g == 0:
            pltpu.make_async_copy(gst, dng_hbm, out_sem.at[2]).start()
        else:
            pltpu.make_async_copy(pre.at[0:CORES], upg_hbm, out_sem.at[3]).start()

    def share(k, own, slots, metas, ret, weighted):
        def of(src, h, cols):
            m = metas[src]
            m = m[:, h * half : (h + 1) * half]
            hit0, hit1 = slots[:, 0:half] == m[0:1, :], slots[:, 0:half] == m[1:2, :]
            v = ret[src, :, cols]
            if not weighted:
                return dot(jnp.where(hit0 | hit1, 1.0, 0.0).astype(BF16), v, TN)
            g = jnp.where(hit0, m[2:3, :], 0.0) + jnp.where(hit1, m[3:4, :], 0.0)
            high = g.astype(BF16)
            low = (g - high.astype(F32)).astype(BF16)
            return dot(high, v, TN) + dot(low, v, TN)
        return of

    def pass_on(k, send, got, src, h, slot, where_d):
        part = send.at[src, halves[h]]
        remote(part, got.at[slot, halves[h]], part_send.at[k, slot, h], part_recv.at[k, slot, h], near(k, where_d)).start()

    def share_with(d, k, own, slots, metas, ret, send, got, out_hbm, weighted):
        of = share(k, own, slots, metas, ret, weighted)
        src = (own + d) % SIDE
        await_bytes(ret.at[src], bwd_recv.at[k, src])
        for h, slot, to in {1: ((1, 1, 1),), 3: ((0, 0, 3),), 2: ((0, 2, 1), (1, 2, 3))}[d]:
            def body(cols, h=h):
                send[src, halves[h], cols] = of(src, h, cols).astype(BF16)

            tiles(body)
            pass_on(k, send, got, src, h, slot, to)

    def hand_on(k, own, slots, metas, ret, send, got, out_hbm, weighted):
        of = share(k, own, slots, metas, ret, weighted)
        ahead, behind = (own + 1) % SIDE, (own + SIDE - 1) % SIDE
        for src, h, slot, d in ((ahead, 0, 1, 1), (behind, 1, 0, SIDE - 1)):
            await_bytes(got.at[2, halves[h]], part_recv.at[k, 2, h])

            def body(cols, src=src, h=h):
                total = of(src, h, cols) + got[2, halves[h], cols].astype(F32)
                send[src, halves[h], cols] = total.astype(BF16)

            tiles(body)
            pass_on(k, send, got, src, h, slot, d)

    def finish(k, own, slots, metas, ret, send, got, out_hbm, weighted):
        of = share(k, own, slots, metas, ret, weighted)
        await_bytes(ret.at[own], bwd_recv.at[k, own])
        for slot in range(2):
            for h in range(2):
                await_bytes(got.at[slot, halves[h]], part_recv.at[k, slot, h])
        for h in range(2):
            def body(cols, h=h):
                total = of(own, h, cols) + got[0, halves[h], cols].astype(F32)
                send[own, halves[h], cols] = (total + got[1, halves[h], cols].astype(F32)).astype(BF16)

            tiles(body)
        pltpu.make_async_copy(send.at[own], out_hbm, out_sem.at[k]).start()

    fwd = (0, z, tok_slots, meta_z, ret_o, recv_t, pmr, mixed_hbm, True)
    bwd = (1, x, cot_slots, meta_x, ret_d, recv_c, pdr, igrad_hbm, False)
    relay_tokens(0)
    relay_cotangents(0)
    hand_over()
    for d in (1, 3, 2):
        relay_tokens(d)
        relay_cotangents(d)
    wup_in.wait()
    wdn_in.wait()
    activate_column()
    cotangents_in(0)
    backward(0)
    for d in (0, 1, 3, 2):
        forward(d)
    cotangents_in(2)
    backward(2)
    for d in (1, 3):
        cotangents_in(d)
    drain()
    weight_grad(0)
    backward(1)
    backward(3)
    weight_grad(1)
    share_with(2, *bwd)
    share_with(1, *fwd)
    share_with(3, *fwd)
    share_with(1, *bwd)
    share_with(3, *bwd)
    share_with(2, *fwd)
    hand_on(*bwd)
    gradients_out(0)
    hand_on(*fwd)
    finish(*bwd)
    gradients_out(1)
    finish(*fwd)

    @pl.loop(0, SIDE)
    def _(j):
        for k, buf in ((0, sbuf_t), (1, sbuf_c)):
            await_bytes(buf.at[j, pl.ds(0, rows - cap)], bwd_send.at[k, j])

    for k, got in ((0, pmr), (1, pdr)):
        for slot in range(SIDE - 1):
            for h in range(2):
                await_bytes(got.at[slot, halves[h]], part_send.at[k, slot, h])

    for g, gbuf in ((0, cotbuf), (1, tokbuf)):
        await_bytes(gbuf.at[0:thirds, :, 0 : width - shard], rs_send.at[g])

    pltpu.make_async_copy(recv_t.at[z], mixed_hbm, out_sem.at[0]).wait()
    pltpu.make_async_copy(recv_c.at[x], igrad_hbm, out_sem.at[1]).wait()
    pltpu.make_async_copy(gst, dng_hbm, out_sem.at[2]).wait()
    pltpu.make_async_copy(pre.at[0:CORES], upg_hbm, out_sem.at[3]).wait()


def copy_kernel(*refs):
    srcs, dsts, bufs, sem = refs[0:4], refs[4:8], refs[8:12], refs[12]
    pieces = []
    for i in range(4):
        first = srcs[i].shape[0] // 2
        pieces += [(i, h, pl.ds(h * first, first)) for h in range(2)]
    for i, h, part in pieces:
        pltpu.make_async_copy(srcs[i].at[part], bufs[i].at[part], sem.at[0, i, h]).start()
    for i, h, part in pieces:
        pltpu.make_async_copy(srcs[i].at[part], bufs[i].at[part], sem.at[0, i, h]).wait()
        pltpu.make_async_copy(bufs[i].at[part], dsts[i].at[part], sem.at[1, i, h]).start()
    for i, h, part in pieces:
        pltpu.make_async_copy(bufs[i].at[part], dsts[i].at[part], sem.at[1, i, h]).wait()


def on_device(tokens, routes, gate_weights, w_up, w_down, cotangent):
    rows, width = tokens.shape
    held, _, hidden = w_up.shape
    shard = width // (SIDE * CORES)
    hbm = pl.BlockSpec(memory_space=pl.ANY)
    vmem = pl.BlockSpec(memory_space=pltpu.VMEM)
    four = pltpu.VMEM((SIDE, rows, width), BF16)
    three = pltpu.VMEM((SIDE - 1, rows, width), BF16)
    dma = pltpu.SemaphoreType.DMA
    results = pl.pallas_call(
        layer_kernel,
        out_shape=(
            jax.ShapeDtypeStruct((rows, width), BF16),
            jax.ShapeDtypeStruct((rows, width), BF16),
            jax.ShapeDtypeStruct((held, shard, hidden), F32),
            jax.ShapeDtypeStruct((held, hidden, shard), F32),
        ),
        in_specs=[hbm, hbm, vmem, vmem, hbm, hbm],
        out_specs=(hbm, hbm, hbm, hbm),
        scratch_shapes=[
            four, four,
            pltpu.VMEM((SIDE, 8, rows), F32), pltpu.VMEM((SIDE, 8, rows), F32),
            four, four, four, four,
            pltpu.VMEM((width, hidden), BF16), pltpu.VMEM((hidden, width), BF16),
            pltpu.VMEM((SIDE, rows, hidden), F32),
            pltpu.VMEM((SIDE, rows, hidden), BF16), pltpu.VMEM((SIDE, rows, hidden), BF16),
            four, four,
            pltpu.VMEM((2, CORES, SIDE, hidden // rows, rows, shard), BF16),
            three, three,
            pltpu.VMEM((CORES, hidden, shard), F32),
            dma((4,)), dma((2, 2, 2)), dma((2, SIDE, 2)), dma((2, 2)),
            dma((2, SIDE)), dma((2, SIDE)), dma((SIDE,)),
            dma((2, SIDE)), dma((2, SIDE)), dma((2, SIDE)), dma((2, SIDE)),
            dma((2,)), dma((2,)), dma((2, SIDE - 1, 2)), dma((2, SIDE - 1, 2)), dma((4,)),
        ],
        compiler_params=pltpu.CompilerParams(
            collective_id=0, has_side_effects=True, vmem_limit_bytes=63 << 20
        ),
    )(tokens, cotangent, routes.T, gate_weights.T, w_up, w_down)
    return pl.pallas_call(
        copy_kernel,
        out_shape=tuple(jax.ShapeDtypeStruct(r.shape, r.dtype) for r in results),
        in_specs=[hbm] * 4,
        out_specs=(hbm,) * 4,
        scratch_shapes=[pltpu.VMEM(r.shape, r.dtype) for r in results] + [dma((2, 4, 2))],
    )(*results)


def solution(mesh):
    rows = P(("dp", "expert"), None)
    held = P("expert", None, None)
    return jax.shard_map(
        on_device,
        mesh=mesh,
        in_specs=(rows, rows, rows, held, held, rows),
        out_specs=(rows, rows, P("expert", "dp", None), P("expert", None, "dp")),
        check_vma=False,
    )
```

```python
import jax
import jax.numpy as jnp
from jax import lax
from jax.experimental import pallas as pl
from jax.experimental.pallas import tpu as pltpu
from jax.sharding import PartitionSpec as P

MESH = pl.DeviceIdType.MESH
SIDE = 4
CORES = 2
F32 = jnp.float32
BF16 = jnp.bfloat16


def dot(a, b, dims):
    return lax.dot_general(a, b, (dims, ((), ())), preferred_element_type=F32)


NN = ((1,), (0,))
NT = ((1,), (1,))
TN = ((0,), (0,))


def sigmoid(v):
    return 1.0 / (1.0 + jnp.exp(-v))


def silu_slope(v, s):
    return (s * (1.0 + v * (1.0 - s))).astype(BF16)


def step_of(j):
    return j ^ (j // 2)


def layer_kernel(
    tok_hbm, cot_hbm, routes, gates, wup_hbm, wdn_hbm,
    mixed, igrad, upg, dng,
    tokbuf, cotbuf, meta_z, meta_x, sbuf_t, sbuf_c, recv_t, recv_c, wu, wd,
    act, dpre, ret_o, ret_d, rs, rs_far, pmr, pdr,
    load_sem, ag_send, ag_recv, hand_send, meta_send, meta_recv, fwd_own,
    fwd_send, fwd_recv, bwd_send, bwd_recv, rs_send, rs_recv, rs_hand, part_send, part_recv,
):
    dp, ex = lax.axis_index("dp"), lax.axis_index("expert")
    y, c = dp // CORES, dp % CORES
    z, x = ex // SIDE, ex % SIDE
    rows, width = tok_hbm.shape
    hidden = wup_hbm.shape[2]
    cap = rows // (SIDE * CORES)
    pair = CORES * cap
    tile = width // SIDE
    shard = width // (SIDE * CORES)
    line = SIDE * CORES
    mine = (x * CORES + c) * cap
    mine_z = (z * CORES + c) * cap

    def device(yy, cc, zz, xx):
        return (yy * CORES + cc, zz * SIDE + xx)

    def x_line(q):
        return (x + q // CORES) % SIDE, (c + q % CORES) % CORES

    def z_line(q):
        return (z + q // CORES) % SIDE, (c + q % CORES) % CORES

    def remote(src, dst, ssem, rsem, where):
        return pltpu.make_async_remote_copy(
            src_ref=src, dst_ref=dst, send_sem=ssem, recv_sem=rsem,
            device_id=where, device_id_type=MESH,
        )

    half = rows // 2
    halves = (pl.ds(0, half), pl.ds(half, half))

    def near(k, d):
        if k == 0:
            return device(y, c, (z + d) % SIDE, x)
        return device(y, c, z, (x + d) % SIDE)

    def await_bytes(ref, sem):
        pltpu.make_async_copy(ref, ref, sem).wait()

    tok_in = pltpu.make_async_copy(tok_hbm, tokbuf.at[z], load_sem.at[0])
    cot_in = pltpu.make_async_copy(cot_hbm, cotbuf.at[x], load_sem.at[1])
    wup_in = pltpu.make_async_copy(wup_hbm.at[c], wu, load_sem.at[2])
    wdn_in = pltpu.make_async_copy(wdn_hbm.at[c], wd, load_sem.at[3])
    tok_in.start()
    cot_in.start()

    barrier = pltpu.get_barrier_semaphore()

    def greet(where):
        pl.semaphore_signal(barrier, inc=1, device_id=where, device_id_type=MESH)

    @pl.loop(1, line)
    def _(q):
        xx, cc = x_line(q)
        greet(device(y, cc, z, xx))

    @pl.loop(CORES, line)
    def _(q):
        zz, cc = z_line(q)
        greet(device(y, cc, zz, x))

    for d in (1, SIDE - 1):
        for core in range(CORES):
            greet(device((y + d) % SIDE, core, z, x))

    r0, r1 = routes[0:1, :], routes[1:2, :]
    experts = line * SIDE
    names = lax.broadcasted_iota(jnp.int32, (experts, rows), 0)
    hit0, hit1 = names == r0, names == r1
    onehot = jnp.where(hit0 | hit1, 1.0, 0.0).astype(BF16)
    earlier = (
        lax.broadcasted_iota(jnp.int32, (rows, rows), 0)
        < lax.broadcasted_iota(jnp.int32, (rows, rows), 1)
    )
    before = dot(onehot, jnp.where(earlier, 1.0, 0.0).astype(BF16), NN)
    slot0 = r0.astype(F32) * cap + jnp.sum(jnp.where(hit0, before, 0.0), axis=0, keepdims=True)
    slot1 = r1.astype(F32) * cap + jnp.sum(jnp.where(hit1, before, 0.0), axis=0, keepdims=True)
    meta = jnp.concatenate(
        [slot0, slot1, gates[0:1, :], gates[1:2, :], jnp.zeros((4, rows), F32)], axis=0
    )
    meta_z[z] = meta
    meta_x[x] = meta

    pl.semaphore_wait(barrier, line - 1 + line - CORES + 2 * CORES)

    @pl.loop(1, SIDE)
    def _(j):
        d = step_of(j)
        to_z, to_x = device(y, c, (z + d) % SIDE, x), device(y, c, z, (x + d) % SIDE)
        remote(meta_z.at[z], meta_z.at[z], meta_send.at[0, d], meta_recv.at[0, z], to_z).start()
        remote(meta_x.at[x], meta_x.at[x], meta_send.at[1, d], meta_recv.at[1, x], to_x).start()

    tok_in.wait()
    cot_in.wait()

    axes = ((0, tokbuf, z), (1, cotbuf, x))
    for first in (True, False):
        for k, buf, own in axes:
            for side, d in ((0, 1), (1, SIDE - 1)):
                h = side if first else 1 - side
                part = buf.at[own, halves[h]]
                remote(part, part, ag_send.at[k, side, h], ag_recv.at[k, own, h], near(k, d)).start()

    wup_in.start()
    wdn_in.start()

    place = lax.broadcasted_iota(jnp.int32, (rows, rows), 0)
    tok_slots = (place + z * rows).astype(F32)
    cot_slots = ((place // pair) * rows + x * pair + place % pair).astype(F32)

    def tiles(body):
        @pl.loop(0, SIDE)
        def _(n):
            body(pl.ds(pl.multiple_of(n * tile, tile), tile))

    def hand_over():
        for k, buf, own in axes:
            for side, back, ahead in ((0, SIDE - 1, 1), (1, 1, SIDE - 1)):
                src = (own + back) % SIDE
                part = buf.at[src, halves[side]]
                await_bytes(part, ag_recv.at[k, src, side])
                remote(part, part, hand_send.at[k, side], ag_recv.at[k, src, side], near(k, ahead)).start()

    def arrived(k, buf, metas, src, d):
        if d != 0:
            await_bytes(metas.at[src], meta_recv.at[k, src])
        if d in (1, 2):
            await_bytes(buf.at[src, halves[0]], ag_recv.at[k, src, 0])
        if d in (SIDE - 1, 2):
            await_bytes(buf.at[src, halves[1]], ag_recv.at[k, src, 1])

    def relay_tokens(d):
        zs = (z + d) % SIDE
        arrived(0, tokbuf, meta_z, zs, d)
        m = meta_z[zs]
        pick = jnp.where((tok_slots == m[0:1, :]) | (tok_slots == m[1:2, :]), 1.0, 0.0).astype(BF16)

        def body(cols):
            sbuf_t[zs, :, cols] = dot(pick, tokbuf[zs, :, cols], NN).astype(BF16)

        tiles(body)

        def send(q, sem):
            xx, cc = x_line(q)
            remote(
                sbuf_t.at[zs, pl.ds((xx * CORES + cc) * cap, cap)],
                recv_t.at[zs, pl.ds(mine, cap)],
                fwd_send.at[0, zs], sem, device(y, cc, z, xx),
            ).start()

        send(1, fwd_own.at[zs])
        pltpu.make_async_copy(
            sbuf_t.at[zs, pl.ds(mine, cap)], recv_t.at[zs, pl.ds(mine, cap)], fwd_own.at[zs]
        ).start()

        @pl.loop(CORES, line)
        def _(q):
            send(q, fwd_recv.at[0, zs])

    def relay_cotangents(d):
        xs = (x + d) % SIDE
        arrived(1, cotbuf, meta_x, xs, d)
        m = meta_x[xs]
        hit0, hit1 = cot_slots == m[0:1, :], cot_slots == m[1:2, :]
        pick = jnp.where(hit0 | hit1, 1.0, 0.0).astype(BF16)
        scale = jnp.sum(
            jnp.where(hit0, m[2:3, :], 0.0) + jnp.where(hit1, m[3:4, :], 0.0), axis=1, keepdims=True
        )

        def body(cols):
            sbuf_c[xs, :, cols] = (dot(pick, cotbuf[xs, :, cols], NN) * scale).astype(BF16)

        tiles(body)

        @pl.loop(1, line)
        def _(q):
            zz, cc = z_line(q)
            remote(
                sbuf_c.at[xs, pl.ds((zz * CORES + cc) * cap, cap)],
                recv_c.at[z, pl.ds((xs * CORES + c) * cap, cap)],
                fwd_send.at[1, xs], fwd_recv.at[1, xs], device(y, cc, zz, x),
            ).start()

        pltpu.make_async_copy(
            sbuf_c.at[xs, pl.ds(mine_z, cap)],
            recv_c.at[z, pl.ds((xs * CORES + c) * cap, cap)],
            fwd_recv.at[1, xs],
        ).start()

    def column(xs):
        return pl.ds(pl.multiple_of(xs * pair, pair), pair)

    def activate_column():
        for d in range(SIDE):
            zs = (z + d) % SIDE
            await_bytes(recv_t.at[zs, column(x)], fwd_own.at[zs])
        v = dot(recv_t[:, column(x), :].reshape(SIDE * pair, width), wu[...], NN)
        dpre[:, column(x), :] = silu_slope(v, sigmoid(v)).reshape(SIDE, pair, hidden)

    def forward(d):
        zs = (z + d) % SIDE
        await_bytes(recv_t.at[zs, 0 : rows - pair], fwd_recv.at[0, zs])
        v = dot(recv_t[zs], wu[...], NN)
        s = sigmoid(v)
        act[zs] = (v * s).astype(BF16)
        done = dpre[zs, column(x), :]
        dpre[zs] = silu_slope(v, s)
        dpre[zs, column(x), :] = done
        await_bytes(sbuf_t.at[zs, pl.ds(0, rows - cap)], fwd_send.at[0, zs])

        def body(cols):
            sbuf_t[zs, :, cols] = dot(act[zs], wd[:, cols], NN).astype(BF16)

        tiles(body)

        @pl.loop(1, line)
        def _(q):
            xx, cc = x_line(q)
            remote(
                sbuf_t.at[zs, pl.ds((xx * CORES + cc) * cap, cap)],
                ret_o.at[zs, pl.ds(mine, cap)],
                bwd_send.at[0, zs], bwd_recv.at[0, zs], device(y, cc, z, xx),
            ).start()

        pltpu.make_async_copy(
            sbuf_t.at[zs, pl.ds(mine, cap)], ret_o.at[zs, pl.ds(mine, cap)], bwd_recv.at[0, zs]
        ).start()

    def cotangents_in(d):
        xs = (x + d) % SIDE
        await_bytes(recv_c.at[:, column(xs)], fwd_recv.at[1, xs])

    def backward(d):
        xs = (x + d) % SIDE
        part = column(xs)
        da = dot(recv_c[:, part, :].reshape(rows, width), wd[...], NT)
        slope = dpre[:, part, :].reshape(rows, hidden).astype(F32)
        dpre[:, part, :] = (da * slope).astype(BF16).reshape(SIDE, pair, hidden)
        await_bytes(sbuf_c.at[xs, pl.ds(0, rows - cap)], fwd_send.at[1, xs])

        def body(cols):
            left = dpre[:, part, :].reshape(rows, hidden)
            sbuf_c[xs, :, cols] = dot(left, wu[cols, :], NT).astype(BF16)

        tiles(body)

        @pl.loop(1, line)
        def _(q):
            zz, cc = z_line(q)
            remote(
                sbuf_c.at[xs, pl.ds((zz * CORES + cc) * cap, cap)],
                ret_d.at[xs, pl.ds(mine_z, cap)],
                bwd_send.at[1, xs], bwd_recv.at[1, xs], device(y, cc, zz, x),
            ).start()

        pltpu.make_async_copy(
            sbuf_c.at[xs, pl.ds(mine_z, cap)], ret_d.at[xs, pl.ds(mine_z, cap)], bwd_recv.at[1, xs]
        ).start()

    def drain():
        @pl.loop(1, SIDE)
        def _(d):
            for k, own, metas in ((0, z, meta_z), (1, x, meta_x)):
                await_bytes(metas.at[own], meta_send.at[k, d])

        for k, buf, own in axes:
            for side, back in ((0, SIDE - 1), (1, 1)):
                for h in range(2):
                    await_bytes(buf.at[own, halves[h]], ag_send.at[k, side, h])
                await_bytes(buf.at[(own + back) % SIDE, halves[side]], hand_send.at[k, side])

    thirds = hidden // rows

    def grad_cols(d, core):
        return pl.ds(pl.multiple_of(((y + d) % SIDE * CORES + core) * shard, shard), shard)

    def send_grad(g, d, core, dst, sem, where):
        gbuf = (cotbuf, tokbuf)[g]
        remote(gbuf.at[0:thirds, :, grad_cols(d, core)], dst, rs_send.at[g], sem, where).start()

    def weight_grad(g):
        left, right, gbuf = ((act, recv_c, cotbuf), (dpre, recv_t, tokbuf))[g]
        ahead, behind = (y + 1) % SIDE, (y + SIDE - 1) % SIDE

        @pl.loop(0, SIDE)
        def _(n):
            yy = (y + 2 + n) % SIDE
            cols = pl.ds(pl.multiple_of(yy * tile, tile), tile)
            r = dot(
                left[...].reshape(SIDE * rows, hidden),
                right[:, :, cols].reshape(SIDE * rows, tile),
                TN,
            )
            gbuf[0:thirds, :, cols] = r.astype(BF16).reshape(thirds, rows, tile)

            @pl.when(n == 0)
            def _():
                send_grad(g, 2, 0, rs_far.at[g, 0], rs_hand.at[g, 0], device(ahead, c, z, x))
                send_grad(g, 2, 1, rs_far.at[g, 1], rs_hand.at[g, 1], device(behind, c, z, x))

        send_grad(g, 1, 1, rs.at[g, c, 1], rs_recv.at[g], device(ahead, 1, z, x))
        send_grad(g, SIDE - 1, 0, rs.at[g, c, 0], rs_recv.at[g], device(behind, 0, z, x))
        send_grad(g, 0, 1 - c, rs.at[g, c, 2], rs_recv.at[g], device(y, 1 - c, z, x))
        pltpu.make_async_copy(
            gbuf.at[0:thirds, :, grad_cols(0, c)], rs.at[g, c, 2], rs_recv.at[g]
        ).start()

    def hand_on_grad(g):
        gbuf = (cotbuf, tokbuf)[g]
        for h, d, slot in ((0, 1, 1), (1, SIDE - 1, 0)):
            await_bytes(rs_far.at[g, h], rs_hand.at[g, h])
            cols = grad_cols(d, h)
            gbuf[0:thirds, :, cols] = (
                gbuf[0:thirds, :, cols].astype(F32) + rs_far[g, h].astype(F32)
            ).astype(BF16)
            send_grad(g, d, h, rs.at[g, c, slot], rs_recv.at[g], device((y + d) % SIDE, h, z, x))

    def gradients_out(g):
        await_bytes(rs.at[g], rs_recv.at[g])

        @pl.loop(0, CORES)
        def _(e):
            total = rs[g, e, 0].astype(F32)
            for part in range(1, SIDE - 1):
                total = total + rs[g, e, part].astype(F32)
            if g == 0:
                dng[e] = total.reshape(hidden, shard)
            else:
                upg[e] = total.reshape(hidden, shard).T

    def share(k, own, slots, metas, ret, weighted):
        def of(src, h, cols):
            m = metas[src]
            m = m[:, h * half : (h + 1) * half]
            hit0, hit1 = slots[:, 0:half] == m[0:1, :], slots[:, 0:half] == m[1:2, :]
            v = ret[src, :, cols]
            if not weighted:
                return dot(jnp.where(hit0 | hit1, 1.0, 0.0).astype(BF16), v, TN)
            g = jnp.where(hit0, m[2:3, :], 0.0) + jnp.where(hit1, m[3:4, :], 0.0)
            high = g.astype(BF16)
            low = (g - high.astype(F32)).astype(BF16)
            return dot(high, v, TN) + dot(low, v, TN)
        return of

    def pass_on(k, send, got, src, h, slot, where_d):
        part = send.at[src, halves[h]]
        remote(part, got.at[slot, halves[h]], part_send.at[k, slot, h], part_recv.at[k, slot, h], near(k, where_d)).start()

    def share_with(d, k, own, slots, metas, ret, send, got, out, weighted):
        of = share(k, own, slots, metas, ret, weighted)
        src = (own + d) % SIDE
        await_bytes(ret.at[src], bwd_recv.at[k, src])
        for h, slot, to in {1: ((1, 1, 1),), 3: ((0, 0, 3),), 2: ((0, 2, 1), (1, 2, 3))}[d]:
            def body(cols, h=h):
                send[src, halves[h], cols] = of(src, h, cols).astype(BF16)

            tiles(body)
            pass_on(k, send, got, src, h, slot, to)

    def hand_on(k, own, slots, metas, ret, send, got, out, weighted):
        of = share(k, own, slots, metas, ret, weighted)
        ahead, behind = (own + 1) % SIDE, (own + SIDE - 1) % SIDE
        for src, h, slot, d in ((ahead, 0, 1, 1), (behind, 1, 0, SIDE - 1)):
            await_bytes(got.at[2, halves[h]], part_recv.at[k, 2, h])

            def body(cols, src=src, h=h):
                total = of(src, h, cols) + got[2, halves[h], cols].astype(F32)
                send[src, halves[h], cols] = total.astype(BF16)

            tiles(body)
            pass_on(k, send, got, src, h, slot, d)

    def own_share(k, own, slots, metas, ret, send, got, out, weighted):
        of = share(k, own, slots, metas, ret, weighted)
        await_bytes(ret.at[own], bwd_recv.at[k, own])

        def body(cols):
            for h in range(2):
                send[own, halves[h], cols] = of(own, h, cols).astype(BF16)

        tiles(body)

    def finish(k, own, slots, metas, ret, send, got, out, weighted):
        for h in ((0, 1), (1, 0))[k]:
            for slot in range(2):
                await_bytes(got.at[slot, halves[h]], part_recv.at[k, slot, h])

        @pl.loop(0, rows // 32)
        def _(n):
            part = pl.ds(pl.multiple_of(n * 32, 32), 32)
            total = send[own, part, :].astype(F32) + got[0, part, :].astype(F32)
            out[part, :] = (total + got[1, part, :].astype(F32)).astype(BF16)

    fwd = (0, z, tok_slots, meta_z, ret_o, recv_t, pmr, mixed, True)
    bwd = (1, x, cot_slots, meta_x, ret_d, recv_c, pdr, igrad, False)
    hand_over()
    relay_tokens(0)
    relay_cotangents(0)
    for d in (1, 3, 2):
        relay_tokens(d)
        relay_cotangents(d)
    wup_in.wait()
    wdn_in.wait()
    activate_column()
    cotangents_in(0)
    backward(0)
    for d in (0, 1, 3, 2):
        forward(d)
    cotangents_in(2)
    backward(2)
    for d in (1, 3):
        cotangents_in(d)
    drain()
    weight_grad(0)
    backward(1)
    backward(3)
    weight_grad(1)
    share_with(2, *bwd)
    hand_on_grad(0)
    share_with(1, *fwd)
    share_with(3, *fwd)
    share_with(1, *bwd)
    share_with(3, *bwd)
    hand_on_grad(1)
    share_with(2, *fwd)
    own_share(*bwd)
    hand_on(*bwd)
    gradients_out(0)
    hand_on(*fwd)
    own_share(*fwd)
    finish(*bwd)
    gradients_out(1)
    finish(*fwd)

    @pl.loop(0, SIDE)
    def _(j):
        for k, buf in ((0, sbuf_t), (1, sbuf_c)):
            await_bytes(buf.at[j, pl.ds(0, rows - cap)], bwd_send.at[k, j])

    for k, got in ((0, pmr), (1, pdr)):
        for slot in range(SIDE - 1):
            for h in range(2):
                await_bytes(got.at[slot, halves[h]], part_send.at[k, slot, h])

    for g, gbuf in ((0, cotbuf), (1, tokbuf)):
        await_bytes(gbuf.at[0:thirds, :, 0 : width - shard], rs_send.at[g])


def on_device(tokens, routes, gate_weights, w_up, w_down, cotangent):
    rows, width = tokens.shape
    held, _, hidden = w_up.shape
    shard = width // (SIDE * CORES)
    hbm = pl.BlockSpec(memory_space=pl.ANY)
    vmem = pl.BlockSpec(memory_space=pltpu.VMEM)
    four = pltpu.VMEM((SIDE, rows, width), BF16)
    three = pltpu.VMEM((SIDE - 1, rows, width), BF16)
    dma = pltpu.SemaphoreType.DMA
    shapes = (
        ((rows, width), BF16), ((rows, width), BF16),
        ((held, shard, hidden), F32), ((held, hidden, shard), F32),
    )
    results = pl.pallas_call(
        layer_kernel,
        out_shape=tuple(pltpu.VMEM(*r) for r in shapes),
        in_specs=[hbm, hbm, vmem, vmem, hbm, hbm],
        out_specs=(vmem,) * 4,
        scratch_shapes=[
            four, four,
            pltpu.VMEM((SIDE, 8, rows), F32), pltpu.VMEM((SIDE, 8, rows), F32),
            four, four, four, four,
            pltpu.VMEM((width, hidden), BF16), pltpu.VMEM((hidden, width), BF16),
            pltpu.VMEM((SIDE, rows, hidden), BF16), pltpu.VMEM((SIDE, rows, hidden), BF16),
            four, four,
            pltpu.VMEM((2, CORES, SIDE - 1, hidden // rows, rows, shard), BF16),
            pltpu.VMEM((2, CORES, hidden // rows, rows, shard), BF16),
            three, three,
            dma((4,)), dma((2, 2, 2)), dma((2, SIDE, 2)), dma((2, 2)),
            dma((2, SIDE)), dma((2, SIDE)), dma((SIDE,)),
            dma((2, SIDE)), dma((2, SIDE)), dma((2, SIDE)), dma((2, SIDE)),
            dma((2,)), dma((2,)), dma((2, CORES)),
            dma((2, SIDE - 1, 2)), dma((2, SIDE - 1, 2)),
        ],
        compiler_params=pltpu.CompilerParams(
            collective_id=0, has_side_effects=True, vmem_limit_bytes=58 << 20
        ),
    )(tokens, cotangent, routes.T, gate_weights.T, w_up, w_down)
    return results


def solution(mesh):
    rows = P(("dp", "expert"), None)
    held = P("expert", None, None)
    return jax.shard_map(
        on_device,
        mesh=mesh,
        in_specs=(rows, rows, rows, held, held, rows),
        out_specs=(rows, rows, P("expert", "dp", None), P("expert", None, "dp")),
        check_vma=False,
    )
```

```python
import jax
import jax.numpy as jnp
from jax import lax
from jax.experimental import pallas as pl
from jax.experimental.pallas import tpu as pltpu
from jax.sharding import PartitionSpec as P

MESH = pl.DeviceIdType.MESH
SIDE = 4
CORES = 2
F32 = jnp.float32
BF16 = jnp.bfloat16


def dot(a, b, dims):
    return lax.dot_general(a, b, (dims, ((), ())), preferred_element_type=F32)


NN = ((1,), (0,))
NT = ((1,), (1,))
TN = ((0,), (0,))


def sigmoid(v):
    return 1.0 / (1.0 + jnp.exp(-v))


def silu_slope(v, s):
    return (s * (1.0 + v * (1.0 - s))).astype(BF16)


def step_of(j):
    return j ^ (j // 2)


def layer_kernel(
    tok_hbm, cot_hbm, routes, gates, wup_hbm, wdn_hbm,
    mixed, igrad, upg, dng,
    tokbuf, cotbuf, meta_z, meta_x, sbuf_t, sbuf_c, recv_t, recv_c, wu, wd,
    act, dpre, ret_o, ret_d, rs, rs_far, pmr, pdr,
    load_sem, ag_send, ag_recv, hand_send, meta_send, meta_recv, fwd_own,
    fwd_send, fwd_recv, bwd_send, bwd_recv, rs_send, rs_recv, rs_hand, part_send, part_recv,
):
    dp, ex = lax.axis_index("dp"), lax.axis_index("expert")
    y, c = dp // CORES, dp % CORES
    z, x = ex // SIDE, ex % SIDE
    rows, width = tok_hbm.shape
    hidden = wup_hbm.shape[2]
    cap = rows // (SIDE * CORES)
    pair = CORES * cap
    tile = width // SIDE
    shard = width // (SIDE * CORES)
    line = SIDE * CORES
    mine = (x * CORES + c) * cap
    mine_z = (z * CORES + c) * cap

    def device(yy, cc, zz, xx):
        return (yy * CORES + cc, zz * SIDE + xx)

    def x_line(q):
        return (x + q // CORES) % SIDE, (c + q % CORES) % CORES

    def z_line(q):
        return (z + q // CORES) % SIDE, (c + q % CORES) % CORES

    def remote(src, dst, ssem, rsem, where):
        return pltpu.make_async_remote_copy(
            src_ref=src, dst_ref=dst, send_sem=ssem, recv_sem=rsem,
            device_id=where, device_id_type=MESH,
        )

    half = rows // 2
    halves = (pl.ds(0, half), pl.ds(half, half))

    def near(k, d):
        if k == 0:
            return device(y, c, (z + d) % SIDE, x)
        return device(y, c, z, (x + d) % SIDE)

    def await_bytes(ref, sem):
        pltpu.make_async_copy(ref, ref, sem).wait()

    tok_in = pltpu.make_async_copy(tok_hbm, tokbuf.at[z], load_sem.at[0])
    cot_in = pltpu.make_async_copy(cot_hbm, cotbuf.at[x], load_sem.at[1])
    wup_in = pltpu.make_async_copy(wup_hbm.at[c], wu, load_sem.at[2])
    wdn_in = pltpu.make_async_copy(wdn_hbm.at[c], wd, load_sem.at[3])
    tok_in.start()
    cot_in.start()

    barrier = pltpu.get_barrier_semaphore()

    def greet(where):
        pl.semaphore_signal(barrier, inc=1, device_id=where, device_id_type=MESH)

    @pl.loop(1, line)
    def _(q):
        xx, cc = x_line(q)
        greet(device(y, cc, z, xx))

    @pl.loop(CORES, line)
    def _(q):
        zz, cc = z_line(q)
        greet(device(y, cc, zz, x))

    for d in (1, SIDE - 1):
        for core in range(CORES):
            greet(device((y + d) % SIDE, core, z, x))

    r0, r1 = routes[0:1, :], routes[1:2, :]
    experts = line * SIDE
    names = lax.broadcasted_iota(jnp.int32, (experts, rows), 0)
    hit0, hit1 = names == r0, names == r1
    onehot = jnp.where(hit0 | hit1, 1.0, 0.0).astype(BF16)
    earlier = (
        lax.broadcasted_iota(jnp.int32, (rows, rows), 0)
        < lax.broadcasted_iota(jnp.int32, (rows, rows), 1)
    )
    before = dot(onehot, jnp.where(earlier, 1.0, 0.0).astype(BF16), NN)
    slot0 = r0.astype(F32) * cap + jnp.sum(jnp.where(hit0, before, 0.0), axis=0, keepdims=True)
    slot1 = r1.astype(F32) * cap + jnp.sum(jnp.where(hit1, before, 0.0), axis=0, keepdims=True)
    meta = jnp.concatenate(
        [slot0, slot1, gates[0:1, :], gates[1:2, :], jnp.zeros((4, rows), F32)], axis=0
    )
    meta_z[z] = meta
    meta_x[x] = meta

    pl.semaphore_wait(barrier, line - 1 + line - CORES + 2 * CORES)

    tok_in.wait()
    cot_in.wait()

    axes = ((0, tokbuf, z), (1, cotbuf, x))
    for first in (True, False):
        for k, buf, own in axes:
            for side, d in ((0, 1), (1, SIDE - 1)):
                h = side if first else 1 - side
                part = buf.at[own, halves[h]]
                remote(part, part, ag_send.at[k, side, h], ag_recv.at[k, own, h], near(k, d)).start()

    @pl.loop(1, SIDE)
    def _(j):
        d = step_of(j)
        to_z, to_x = device(y, c, (z + d) % SIDE, x), device(y, c, z, (x + d) % SIDE)
        remote(meta_z.at[z], meta_z.at[z], meta_send.at[0, d], meta_recv.at[0, z], to_z).start()
        remote(meta_x.at[x], meta_x.at[x], meta_send.at[1, d], meta_recv.at[1, x], to_x).start()

    wup_in.start()
    wdn_in.start()

    place = lax.broadcasted_iota(jnp.int32, (rows, rows), 0)
    tok_slots = (place + z * rows).astype(F32)
    cot_slots = ((place // pair) * rows + x * pair + place % pair).astype(F32)

    def tiles(body):
        @pl.loop(0, SIDE)
        def _(n):
            body(pl.ds(pl.multiple_of(n * tile, tile), tile))

    def hand_over():
        for k, buf, own in axes:
            for side, back, ahead in ((0, SIDE - 1, 1), (1, 1, SIDE - 1)):
                src = (own + back) % SIDE
                part = buf.at[src, halves[side]]
                await_bytes(part, ag_recv.at[k, src, side])
                remote(part, part, hand_send.at[k, side], ag_recv.at[k, src, side], near(k, ahead)).start()

    def arrived(k, buf, metas, src, d):
        if d != 0:
            await_bytes(metas.at[src], meta_recv.at[k, src])
        if d in (1, 2):
            await_bytes(buf.at[src, halves[0]], ag_recv.at[k, src, 0])
        if d in (SIDE - 1, 2):
            await_bytes(buf.at[src, halves[1]], ag_recv.at[k, src, 1])

    def relay_tokens(d):
        zs = (z + d) % SIDE
        arrived(0, tokbuf, meta_z, zs, d)
        m = meta_z[zs]
        pick = jnp.where((tok_slots == m[0:1, :]) | (tok_slots == m[1:2, :]), 1.0, 0.0).astype(BF16)

        def body(cols):
            sbuf_t[zs, :, cols] = dot(pick, tokbuf[zs, :, cols], NN).astype(BF16)

        tiles(body)

        def send(q, sem):
            xx, cc = x_line(q)
            remote(
                sbuf_t.at[zs, pl.ds((xx * CORES + cc) * cap, cap)],
                recv_t.at[zs, pl.ds(mine, cap)],
                fwd_send.at[0, zs], sem, device(y, cc, z, xx),
            ).start()

        send(1, fwd_own.at[zs])
        pltpu.make_async_copy(
            sbuf_t.at[zs, pl.ds(mine, cap)], recv_t.at[zs, pl.ds(mine, cap)], fwd_own.at[zs]
        ).start()

        @pl.loop(CORES, line)
        def _(q):
            send(q, fwd_recv.at[0, zs])

    def relay_cotangents(d):
        xs = (x + d) % SIDE
        arrived(1, cotbuf, meta_x, xs, d)
        m = meta_x[xs]
        hit0, hit1 = cot_slots == m[0:1, :], cot_slots == m[1:2, :]
        pick = jnp.where(hit0 | hit1, 1.0, 0.0).astype(BF16)
        scale = jnp.sum(
            jnp.where(hit0, m[2:3, :], 0.0) + jnp.where(hit1, m[3:4, :], 0.0), axis=1, keepdims=True
        )

        def body(cols):
            sbuf_c[xs, :, cols] = (dot(pick, cotbuf[xs, :, cols], NN) * scale).astype(BF16)

        tiles(body)

        @pl.loop(1, line)
        def _(q):
            zz, cc = z_line(q)
            remote(
                sbuf_c.at[xs, pl.ds((zz * CORES + cc) * cap, cap)],
                recv_c.at[z, pl.ds((xs * CORES + c) * cap, cap)],
                fwd_send.at[1, xs], fwd_recv.at[1, xs], device(y, cc, zz, x),
            ).start()

        pltpu.make_async_copy(
            sbuf_c.at[xs, pl.ds(mine_z, cap)],
            recv_c.at[z, pl.ds((xs * CORES + c) * cap, cap)],
            fwd_recv.at[1, xs],
        ).start()

    def column(xs):
        return pl.ds(pl.multiple_of(xs * pair, pair), pair)

    def activate_column():
        for d in range(SIDE):
            zs = (z + d) % SIDE
            await_bytes(recv_t.at[zs, column(x)], fwd_own.at[zs])
        v = dot(recv_t[:, column(x), :].reshape(SIDE * pair, width), wu[...], NN)
        dpre[:, column(x), :] = silu_slope(v, sigmoid(v)).reshape(SIDE, pair, hidden)

    def forward(d):
        zs = (z + d) % SIDE
        await_bytes(recv_t.at[zs, 0 : rows - pair], fwd_recv.at[0, zs])
        v = dot(recv_t[zs], wu[...], NN)
        s = sigmoid(v)
        act[zs] = (v * s).astype(BF16)
        done = dpre[zs, column(x), :]
        dpre[zs] = silu_slope(v, s)
        dpre[zs, column(x), :] = done
        await_bytes(sbuf_t.at[zs, pl.ds(0, rows - cap)], fwd_send.at[0, zs])

        def body(cols):
            sbuf_t[zs, :, cols] = dot(act[zs], wd[:, cols], NN).astype(BF16)

        tiles(body)

        @pl.loop(1, line)
        def _(q):
            xx, cc = x_line(q)
            remote(
                sbuf_t.at[zs, pl.ds((xx * CORES + cc) * cap, cap)],
                ret_o.at[zs, pl.ds(mine, cap)],
                bwd_send.at[0, zs], bwd_recv.at[0, zs], device(y, cc, z, xx),
            ).start()

        pltpu.make_async_copy(
            sbuf_t.at[zs, pl.ds(mine, cap)], ret_o.at[zs, pl.ds(mine, cap)], bwd_recv.at[0, zs]
        ).start()

    def cotangents_in(d):
        xs = (x + d) % SIDE
        await_bytes(recv_c.at[:, column(xs)], fwd_recv.at[1, xs])

    def backward(d):
        xs = (x + d) % SIDE
        part = column(xs)
        da = dot(recv_c[:, part, :].reshape(rows, width), wd[...], NT)
        slope = dpre[:, part, :].reshape(rows, hidden).astype(F32)
        dpre[:, part, :] = (da * slope).astype(BF16).reshape(SIDE, pair, hidden)
        await_bytes(sbuf_c.at[xs, pl.ds(0, rows - cap)], fwd_send.at[1, xs])

        def body(cols):
            left = dpre[:, part, :].reshape(rows, hidden)
            sbuf_c[xs, :, cols] = dot(left, wu[cols, :], NT).astype(BF16)

        tiles(body)

        @pl.loop(1, line)
        def _(q):
            zz, cc = z_line(q)
            remote(
                sbuf_c.at[xs, pl.ds((zz * CORES + cc) * cap, cap)],
                ret_d.at[xs, pl.ds(mine_z, cap)],
                bwd_send.at[1, xs], bwd_recv.at[1, xs], device(y, cc, zz, x),
            ).start()

        pltpu.make_async_copy(
            sbuf_c.at[xs, pl.ds(mine_z, cap)], ret_d.at[xs, pl.ds(mine_z, cap)], bwd_recv.at[1, xs]
        ).start()

    def drain():
        @pl.loop(1, SIDE)
        def _(d):
            for k, own, metas in ((0, z, meta_z), (1, x, meta_x)):
                await_bytes(metas.at[own], meta_send.at[k, d])

        for k, buf, own in axes:
            for side, back in ((0, SIDE - 1), (1, 1)):
                for h in range(2):
                    await_bytes(buf.at[own, halves[h]], ag_send.at[k, side, h])
                await_bytes(buf.at[(own + back) % SIDE, halves[side]], hand_send.at[k, side])

    thirds = hidden // rows

    def grad_cols(d, core):
        return pl.ds(pl.multiple_of(((y + d) % SIDE * CORES + core) * shard, shard), shard)

    def send_grad(g, d, core, dst, sem, where):
        gbuf = (cotbuf, tokbuf)[g]
        remote(gbuf.at[0:thirds, :, grad_cols(d, core)], dst, rs_send.at[g], sem, where).start()

    def weight_grad(g):
        left, right, gbuf = ((act, recv_c, cotbuf), (dpre, recv_t, tokbuf))[g]
        ahead, behind = (y + 1) % SIDE, (y + SIDE - 1) % SIDE

        @pl.loop(0, SIDE)
        def _(n):
            yy = (y + 2 + n) % SIDE
            cols = pl.ds(pl.multiple_of(yy * tile, tile), tile)
            r = dot(
                left[...].reshape(SIDE * rows, hidden),
                right[:, :, cols].reshape(SIDE * rows, tile),
                TN,
            )
            gbuf[0:thirds, :, cols] = r.astype(BF16).reshape(thirds, rows, tile)

            @pl.when(n == 0)
            def _():
                send_grad(g, 2, 0, rs_far.at[g, 0], rs_hand.at[g, 0], device(ahead, c, z, x))
                send_grad(g, 2, 1, rs_far.at[g, 1], rs_hand.at[g, 1], device(behind, c, z, x))

        send_grad(g, 1, 1, rs.at[g, c, 1], rs_recv.at[g], device(ahead, 1, z, x))
        send_grad(g, SIDE - 1, 0, rs.at[g, c, 0], rs_recv.at[g], device(behind, 0, z, x))
        send_grad(g, 0, 1 - c, rs.at[g, c, 2], rs_recv.at[g], device(y, 1 - c, z, x))
        pltpu.make_async_copy(
            gbuf.at[0:thirds, :, grad_cols(0, c)], rs.at[g, c, 2], rs_recv.at[g]
        ).start()

    def hand_on_grad(g):
        gbuf = (cotbuf, tokbuf)[g]
        for h, d, slot in ((0, 1, 1), (1, SIDE - 1, 0)):
            await_bytes(rs_far.at[g, h], rs_hand.at[g, h])
            cols = grad_cols(d, h)
            gbuf[0:thirds, :, cols] = (
                gbuf[0:thirds, :, cols].astype(F32) + rs_far[g, h].astype(F32)
            ).astype(BF16)
            send_grad(g, d, h, rs.at[g, c, slot], rs_recv.at[g], device((y + d) % SIDE, h, z, x))

    def gradients_out(g):
        await_bytes(rs.at[g], rs_recv.at[g])

        @pl.loop(0, CORES)
        def _(e):
            total = rs[g, e, 0].astype(F32)
            for part in range(1, SIDE - 1):
                total = total + rs[g, e, part].astype(F32)
            if g == 0:
                dng[e] = total.reshape(hidden, shard)
            else:
                upg[e] = total.reshape(hidden, shard).T

    def share(k, own, slots, metas, ret, weighted):
        def of(src, h, cols):
            m = metas[src]
            m = m[:, h * half : (h + 1) * half]
            hit0, hit1 = slots[:, 0:half] == m[0:1, :], slots[:, 0:half] == m[1:2, :]
            v = ret[src, :, cols]
            if not weighted:
                return dot(jnp.where(hit0 | hit1, 1.0, 0.0).astype(BF16), v, TN)
            g = jnp.where(hit0, m[2:3, :], 0.0) + jnp.where(hit1, m[3:4, :], 0.0)
            high = g.astype(BF16)
            low = (g - high.astype(F32)).astype(BF16)
            return dot(high, v, TN) + dot(low, v, TN)
        return of

    def pass_on(k, send, got, src, h, slot, where_d):
        part = send.at[src, halves[h]]
        remote(part, got.at[slot, halves[h]], part_send.at[k, slot, h], part_recv.at[k, slot, h], near(k, where_d)).start()

    def share_with(d, k, own, slots, metas, ret, send, got, out, weighted):
        of = share(k, own, slots, metas, ret, weighted)
        src = (own + d) % SIDE
        await_bytes(ret.at[src], bwd_recv.at[k, src])
        for h, slot, to in {1: ((1, 1, 1),), 3: ((0, 0, 3),), 2: ((0, 2, 1), (1, 2, 3))}[d]:
            def body(cols, h=h):
                send[src, halves[h], cols] = of(src, h, cols).astype(BF16)

            tiles(body)
            pass_on(k, send, got, src, h, slot, to)

    def hand_on(k, own, slots, metas, ret, send, got, out, weighted):
        of = share(k, own, slots, metas, ret, weighted)
        ahead, behind = (own + 1) % SIDE, (own + SIDE - 1) % SIDE
        for src, h, slot, d in ((ahead, 0, 1, 1), (behind, 1, 0, SIDE - 1)):
            await_bytes(got.at[2, halves[h]], part_recv.at[k, 2, h])

            def body(cols, src=src, h=h):
                total = of(src, h, cols) + got[2, halves[h], cols].astype(F32)
                send[src, halves[h], cols] = total.astype(BF16)

            tiles(body)
            pass_on(k, send, got, src, h, slot, d)

    def own_share(k, own, slots, metas, ret, send, got, out, weighted):
        of = share(k, own, slots, metas, ret, weighted)
        await_bytes(ret.at[own], bwd_recv.at[k, own])

        def body(cols):
            for h in range(2):
                send[own, halves[h], cols] = of(own, h, cols).astype(BF16)

        tiles(body)

    def finish(k, own, slots, metas, ret, send, got, out, weighted):
        for h in ((0, 1), (1, 0))[k]:
            for slot in range(2):
                await_bytes(got.at[slot, halves[h]], part_recv.at[k, slot, h])

        @pl.loop(0, rows // 32)
        def _(n):
            part = pl.ds(pl.multiple_of(n * 32, 32), 32)
            total = send[own, part, :].astype(F32) + got[0, part, :].astype(F32)
            out[part, :] = (total + got[1, part, :].astype(F32)).astype(BF16)

    fwd = (0, z, tok_slots, meta_z, ret_o, recv_t, pmr, mixed, True)
    bwd = (1, x, cot_slots, meta_x, ret_d, recv_c, pdr, igrad, False)
    hand_over()
    relay_tokens(0)
    relay_cotangents(0)
    for d in (1, 3, 2):
        relay_tokens(d)
        relay_cotangents(d)
    wup_in.wait()
    wdn_in.wait()
    activate_column()
    cotangents_in(0)
    backward(0)
    for d in (0, 1, 3, 2):
        forward(d)
    cotangents_in(2)
    backward(2)
    for d in (1, 3):
        cotangents_in(d)
    drain()
    weight_grad(0)
    backward(1)
    backward(3)
    weight_grad(1)
    share_with(2, *bwd)
    hand_on_grad(0)
    share_with(1, *fwd)
    share_with(3, *fwd)
    share_with(1, *bwd)
    share_with(3, *bwd)
    hand_on_grad(1)
    share_with(2, *fwd)
    own_share(*bwd)
    hand_on(*bwd)
    gradients_out(0)
    hand_on(*fwd)
    own_share(*fwd)
    finish(*bwd)
    gradients_out(1)
    finish(*fwd)

    @pl.loop(0, SIDE)
    def _(j):
        for k, buf in ((0, sbuf_t), (1, sbuf_c)):
            await_bytes(buf.at[j, pl.ds(0, rows - cap)], bwd_send.at[k, j])

    for k, got in ((0, pmr), (1, pdr)):
        for slot in range(SIDE - 1):
            for h in range(2):
                await_bytes(got.at[slot, halves[h]], part_send.at[k, slot, h])

    for g, gbuf in ((0, cotbuf), (1, tokbuf)):
        await_bytes(gbuf.at[0:thirds, :, 0 : width - shard], rs_send.at[g])


def copy_kernel(*refs):
    srcs, dsts, sem = refs[0:4], refs[4:8], refs[8]
    copies = []
    for i in range(4):
        first = srcs[i].shape[0] // 2
        for h in range(2):
            part = pl.ds(h * first, first)
            copies.append(pltpu.make_async_copy(srcs[i].at[part], dsts[i].at[part], sem.at[i, h]))
    for copy in copies:
        copy.start()
    for copy in copies:
        copy.wait()


def on_device(tokens, routes, gate_weights, w_up, w_down, cotangent):
    rows, width = tokens.shape
    held, _, hidden = w_up.shape
    shard = width // (SIDE * CORES)
    hbm = pl.BlockSpec(memory_space=pl.ANY)
    vmem = pl.BlockSpec(memory_space=pltpu.VMEM)
    four = pltpu.VMEM((SIDE, rows, width), BF16)
    three = pltpu.VMEM((SIDE - 1, rows, width), BF16)
    dma = pltpu.SemaphoreType.DMA
    shapes = (
        ((rows, width), BF16), ((rows, width), BF16),
        ((held, shard, hidden), F32), ((held, hidden, shard), F32),
    )
    results = pl.pallas_call(
        layer_kernel,
        out_shape=tuple(pltpu.VMEM(*r) for r in shapes),
        in_specs=[hbm, hbm, vmem, vmem, hbm, hbm],
        out_specs=(vmem,) * 4,
        scratch_shapes=[
            four, four,
            pltpu.VMEM((SIDE, 8, rows), F32), pltpu.VMEM((SIDE, 8, rows), F32),
            four, four, four, four,
            pltpu.VMEM((width, hidden), BF16), pltpu.VMEM((hidden, width), BF16),
            pltpu.VMEM((SIDE, rows, hidden), BF16), pltpu.VMEM((SIDE, rows, hidden), BF16),
            four, four,
            pltpu.VMEM((2, CORES, SIDE - 1, hidden // rows, rows, shard), BF16),
            pltpu.VMEM((2, CORES, hidden // rows, rows, shard), BF16),
            three, three,
            dma((4,)), dma((2, 2, 2)), dma((2, SIDE, 2)), dma((2, 2)),
            dma((2, SIDE)), dma((2, SIDE)), dma((SIDE,)),
            dma((2, SIDE)), dma((2, SIDE)), dma((2, SIDE)), dma((2, SIDE)),
            dma((2,)), dma((2,)), dma((2, CORES)),
            dma((2, SIDE - 1, 2)), dma((2, SIDE - 1, 2)),
        ],
        compiler_params=pltpu.CompilerParams(
            collective_id=0, has_side_effects=True, vmem_limit_bytes=58 << 20
        ),
    )(tokens, cotangent, routes.T, gate_weights.T, w_up, w_down)
    return pl.pallas_call(
        copy_kernel,
        out_shape=tuple(jax.ShapeDtypeStruct(*r) for r in shapes),
        in_specs=[vmem] * 4,
        out_specs=(hbm,) * 4,
        scratch_shapes=[dma((4, 2))],
        compiler_params=pltpu.CompilerParams(vmem_limit_bytes=8 << 20),
    )(*(pltpu.with_memory_space_constraint(r, pltpu.VMEM) for r in results))


def solution(mesh):
    rows = P(("dp", "expert"), None)
    held = P("expert", None, None)
    return jax.shard_map(
        on_device,
        mesh=mesh,
        in_specs=(rows, rows, rows, held, held, rows),
        out_specs=(rows, rows, P("expert", "dp", None), P("expert", None, "dp")),
        check_vma=False,
    )
```
